32 devices in a mesh: wave: 16 (over z, y, core), lev: 2 (over x).
Axes of the slice: x: 2, y: 2, z: 4, core: 2. Of those that a mesh axis runs over, the one named last changes fastest.
Arguments:
- control: bfloat16 [2, 256, 256, 2, 512], P(None, 'wave', 'lev'), may hold values from -6 to 6
- wave_of_slot: int32 [256], replicated, may hold values from 0 to 255, each once
- legendre: bfloat16 [256, 256, 256], P('wave', 'lev'), may hold values from -0.375 to 0.375
- vertical: bfloat16 [4, 4, 128, 128], replicated, may hold values from -0.5 to 0.5
- points: int32 [256], P('wave'), may hold values from 128 to 512
- lat_band: int32 [256], P('wave'), may hold values from 0 to 7, never falling along the last dimension, each value on 1 to 64 neighbouring positions
- grid_scale: float32 [8, 512], P(None, 'lev'), may hold values from 0.5 to 2
- obs_weight: bfloat16 [256, 512, 512], P('wave', 'lev'), may hold values from 0.19921875 to 1
Outputs:
- increment: bfloat16 [2, 256, 512, 512], P(None, 'wave', 'lev')
- gradient: bfloat16 [2, 256, 256, 2, 512], P(None, 'wave', 'lev')
The draws below stay inside these ranges and needn't reach their ends.
Inputs may be any that keep to these rules, and one draw needn't show every extreme that they name: `wave_of_slot`: each zonal wavenumber 0 to 255 stands in exactly one slot. `lat_band`: band numbers never fall from one latitude to the next, and each band covers 1 to 64 latitudes.
All inputs are finite; a program needn't handle non-finite values.
Results may differ from the reference program's by a relative error of at most 0.007.
Values may be sent and summed in bfloat16 or wider, within the bound.
No kernel may reach another device: no remote copies, remote signals or barrier semaphores. Data moves between devices by JAX's collectives and lax.ppermute only.
A program may use at most 192 MiB of HBM per device.

```python
import math
import jax
import jax.numpy as jnp
import numpy as np

WAVES = 256
LATITUDES = 256
LONGITUDES = 512
LEVELS = 128
VARIABLES = 4
COV_BANDS = 4
LAT_BANDS = 8
MEMBERS = 2
COLUMNS = 512


def plant(drawn, own_key, least, top_value):
    index_at = [jax.random.randint(jax.random.fold_in(own_key, axis), (), 0, length) for axis, length in enumerate(drawn.shape)]
    widest = drawn.shape.index(max(drawn.shape))
    next_to = index_at[:widest] + [(index_at[widest] + 1) % drawn.shape[widest]] + index_at[widest + 1:]
    return drawn.at[tuple(index_at)].set(least).at[tuple(next_to)].set(top_value)


def level_of(stream_key, extent, shards, least, high):
    gain, own = 1.0, jax.random.fold_in(stream_key, 6)
    for position, blocks in shards:
        steps = jnp.exp(jax.random.uniform(jax.random.fold_in(own, position), (blocks,), jnp.float32, least / len(shards), high / len(shards)))
        gain = gain * jnp.repeat(steps, extent[position] // blocks).reshape([-1 if axis == position else 1 for axis in range(len(extent))])
    return gain


def length_profile(count, total, most, skew):
    portions = [(1 << 20) // math.isqrt(rank ** skew) + 1 for rank in range(2, count + 1)]
    rest, holding = total - most - (count - 1), [1] * (count - 1)
    while rest > 0:
        candidates = [i for i in range(count - 1) if holding[i] < most]
        whole, remaining = sum([portions[i] for i in candidates]), rest
        for i in candidates:
            more = min(most - holding[i], max(1, remaining * portions[i] // whole), rest)
            holding[i] = holding[i] + more
            rest = rest - more
    return np.array([most] + holding)


def ragged_sizes(rng, count, total, reach, slope):
    if count == 2:
        one = jax.random.randint(rng, (), max(1, total - reach), min(reach, total - 1) + 1)
        return jnp.stack([one, total - one])
    tallies = jnp.asarray(length_profile(count, total, reach, slope), jnp.int32)
    couples = (count - 1) // 2
    donor, receiver = tallies[1:1 + 2 * couples:2], tallies[2:2 + 2 * couples:2]
    slack = jnp.minimum(donor - 1, reach - receiver)
    passed = jax.random.randint(jax.random.fold_in(rng, 1), (couples,), 0, 1 << 20) % (slack + 1)
    tallies = tallies.at[1:1 + 2 * couples:2].set(donor - passed).at[2:2 + 2 * couples:2].set(receiver + passed)
    return tallies[jax.random.permutation(jax.random.fold_in(rng, 2), count)]


def scatter_about(key, dims, spread, most, pieces=(), held_as=jnp.bfloat16):
    drawn = jax.random.normal(key, dims, jnp.float32) * spread
    if len(pieces) > 0:
        drawn = level_of(key, dims, pieces, -0.22, 0.18) * drawn
    return jnp.clip(drawn, min=-most, max=most).astype(held_as)


def setup_inputs(seed: int = 0) -> dict:
    splits = jax.random.split(jax.random.key(seed), 9)
    return {
        "control": scatter_about(splits[0], (MEMBERS, WAVES, WAVES, 2, COLUMNS), 1.0, 6.0, ((1, 16), (2, 2))),
        "wave_of_slot": jax.random.permutation(splits[1], WAVES).astype(jnp.int32),
        "legendre": scatter_about(splits[2], (WAVES, WAVES, LATITUDES), WAVES ** -0.5, 0.375, ((0, 16), (1, 2))),
        "vertical": scatter_about(splits[3], (COV_BANDS, VARIABLES, LEVELS, LEVELS), LEVELS ** -0.5, 0.5),
        "points": plant(jax.random.randint(splits[4], (LATITUDES,), LONGITUDES // 4, LONGITUDES + 1), jax.random.fold_in(splits[4], 1), LONGITUDES // 4, LONGITUDES).astype(jnp.int32),
        "lat_band": jnp.searchsorted(jnp.cumsum(ragged_sizes(splits[5], LAT_BANDS, LATITUDES, 2 * LATITUDES // LAT_BANDS, 1)), jnp.arange(LATITUDES), side="right").astype(jnp.int32),
        "grid_scale": jnp.clip(jnp.exp(math.log(2.0) - 1.3862944 * jax.random.uniform(splits[6], (LAT_BANDS, COLUMNS), jnp.float32) ** level_of(splits[6], (LAT_BANDS, COLUMNS), ((1, 2),), -0.2, 0.2)), 0.5, 2.0),
        "obs_weight": jnp.clip(jnp.exp(math.log(1.0) - 1.6133518 * jax.random.uniform(splits[7], (LATITUDES, COLUMNS, LONGITUDES), jnp.float32) ** level_of(splits[7], (LATITUDES, COLUMNS, LONGITUDES), ((0, 16), (1, 2)), -0.2, 0.2)), 0.19921875, 1.0).astype(jnp.bfloat16),
    }


def fourier_table(wave_ids, lat_points):
    lon_index = jnp.arange(LONGITUDES, dtype=jnp.int32)
    remainder = wave_ids[None, :, None] * lon_index[None, None, :] % lat_points[:, None, None]
    angles = 2.0 * math.pi * remainder.astype(jnp.float32) / lat_points.astype(jnp.float32)[:, None, None]
    factor = jnp.where(wave_ids == 0, 1.0, 2.0).astype(jnp.float32) / math.sqrt(4.0 * WAVES)
    inside = lon_index[None, None, :] < lat_points[:, None, None]
    cosine = jnp.where(inside, factor[None, :, None] * jnp.cos(angles), 0.0)
    sine = jnp.where(inside, -factor[None, :, None] * jnp.sin(angles), 0.0)
    return jnp.stack([cosine, sine], axis=2).astype(jnp.bfloat16)

def vertical_apply(field, vertical, live_rows, band_of, forward):
    shaped = field.astype(jnp.float32).reshape(WAVES, WAVES, 2, VARIABLES, LEVELS)
    matrices = vertical.astype(jnp.float32)
    form = 'skpam,alm->skpal' if forward else 'skpal,alm->skpam'
    summed = jnp.zeros(shaped.shape, jnp.float32)
    for index_band in range(COV_BANDS):
        partial_value = jnp.einsum(form, shaped, matrices[index_band])
        chosen = live_rows & (band_of == index_band)
        summed = summed + jnp.where(chosen[:, :, None, None, None], partial_value, 0.0)
    return summed.reshape(WAVES, WAVES, 2, COLUMNS).astype(jnp.bfloat16)

def reference(control, wave_of_slot, legendre, vertical, points, lat_band, grid_scale, obs_weight):
    row_index = jnp.arange(WAVES, dtype=jnp.int32)
    totals_n = wave_of_slot[:, None] + row_index[None, :]
    live_rows = totals_n <= WAVES - 1
    band_of = jnp.minimum(totals_n * COV_BANDS // WAVES, COV_BANDS - 1)
    fourier = fourier_table(wave_of_slot, points).astype(jnp.float32)
    table32 = legendre.astype(jnp.float32)
    lat_scale = grid_scale[lat_band]
    weight32 = obs_weight.astype(jnp.float32)
    increments = []
    gradients = []
    for member in range(MEMBERS):
        spectral = vertical_apply(control[member], vertical, live_rows, band_of, True)
        flat = spectral.astype(jnp.float32).reshape(WAVES, WAVES, 2 * COLUMNS)
        coeffs = jnp.einsum('skt,skq->stq', table32, flat).astype(jnp.bfloat16)
        coeffs32 = coeffs.astype(jnp.float32).reshape(WAVES, LATITUDES, 2, COLUMNS)
        synthesis = jnp.einsum('tspj,stpc->tcj', fourier, coeffs32)
        increment = (synthesis * lat_scale[:, :, None]).astype(jnp.bfloat16)
        weighted = (increment.astype(jnp.float32) * weight32 * lat_scale[:, :, None]).astype(jnp.bfloat16)
        adjoint_fourier = jnp.einsum('tspj,tcj->tspc', fourier, weighted.astype(jnp.float32)).astype(jnp.bfloat16)
        adjoint_flat = adjoint_fourier.astype(jnp.float32).reshape(LATITUDES, WAVES, 2 * COLUMNS)
        adjoint_coeffs = jnp.einsum('skt,tsq->skq', table32, adjoint_flat).astype(jnp.bfloat16)
        adjoint_coeffs = adjoint_coeffs.reshape(WAVES, WAVES, 2, COLUMNS)
        gradient = vertical_apply(adjoint_coeffs, vertical, live_rows, band_of, False)
        increments.append(increment)
        gradients.append(gradient)
    return (jnp.stack(increments, axis=0), jnp.stack(gradients, axis=0))
```

```python
import functools
import math

import jax
import jax.numpy as jnp
from jax import lax
from jax.experimental import pallas as pl
from jax.experimental.pallas import tpu as pltpu
from jax.sharding import PartitionSpec as P

WAVES = 256
LONGITUDES = 512
LEVELS = 128
VARIABLES = 4
COV_BANDS = 4
LANES = 128

BF16 = jnp.bfloat16
F32 = jnp.float32


def params(*semantics):
    return pltpu.CompilerParams(dimension_semantics=semantics, vmem_limit_bytes=56 << 20)


def cost(flops, nbytes):
    return pl.CostEstimate(flops=int(flops), bytes_accessed=int(nbytes), transcendentals=0)


def dot(a, b, contract):
    return lax.dot_general(a, b, (contract, ((), ())), preferred_element_type=F32)


def band_masked(rows, first_total):
    row_total = first_total + lax.broadcasted_iota(jnp.int32, rows.shape, 0) // 2
    width = WAVES // COV_BANDS
    parts = []
    for band in range(COV_BANDS):
        inside = (row_total >= band * width) & (row_total < (band + 1) * width)
        parts.append(jnp.where(inside, rows, jnp.zeros_like(rows)))
    return jnp.concatenate(parts, axis=1)


def vertical_fwd_body(info, waves, xo, xs, vo, vs, own, send, scratch):
    rows_dev = own.shape[1]
    first_total = waves[pl.program_id(0)] + info[0] * rows_dev
    for x, v, out in ((xo, vo, own), (xs, vs, send)):
        rows = x[0, 0].reshape(2 * rows_dev, LEVELS)
        matrix = jnp.concatenate([v[band, 0] for band in range(COV_BANDS)], axis=1)
        scratch[...] = dot(band_masked(rows, first_total), matrix, ((1,), (1,)))
        for part in range(2):
            out[0, :, part * LEVELS : (part + 1) * LEVELS] = scratch[
                pl.ds(part, rows_dev, stride=2), :
            ].astype(BF16)


def vertical_fwd(control, vertical, info, waves, member, sub, subs):
    _, slots, rows_dev, _, _ = control.shape
    block = (1, 1, rows_dev, 2, LEVELS)
    vblock = (COV_BANDS, 1, LEVELS, LEVELS)
    oblock = (1, rows_dev, 2 * LEVELS)
    mine = lambda info: info[0] * subs + sub
    other = lambda info: (1 - info[0]) * subs + sub
    shape = jax.ShapeDtypeStruct((slots, rows_dev, 2 * LEVELS), BF16)
    return pl.pallas_call(
        vertical_fwd_body,
        grid_spec=pltpu.PrefetchScalarGridSpec(
            num_scalar_prefetch=2,
            grid=(slots,),
            in_specs=[
                pl.BlockSpec(block, lambda s, info, w: (member, s, 0, 0, mine(info))),
                pl.BlockSpec(block, lambda s, info, w: (member, s, 0, 0, other(info))),
                pl.BlockSpec(vblock, lambda s, info, w: (0, mine(info), 0, 0)),
                pl.BlockSpec(vblock, lambda s, info, w: (0, other(info), 0, 0)),
            ],
            out_specs=[
                pl.BlockSpec(oblock, lambda s, info, w: (s, 0, 0)),
                pl.BlockSpec(oblock, lambda s, info, w: (s, 0, 0)),
            ],
            scratch_shapes=[pltpu.VMEM((2 * rows_dev, LEVELS), F32)],
        ),
        out_shape=[shape, shape],
        compiler_params=params("arbitrary"),
        cost_estimate=cost(16 * slots * rows_dev * COV_BANDS * LEVELS * LEVELS, 8 * slots * rows_dev * 256),
        name="vertical_fwd",
    )(info, waves, control, control, vertical, vertical)


def vertical_adj_body(info, waves, own, other, v, *rest):
    out, scratch = rest[-2:]
    rows_dev = own.shape[1]
    first_total = waves[pl.program_id(0)] + info[0] * rows_dev

    def run(block):
        for part in range(2):
            scratch[pl.ds(part, rows_dev, stride=2), :] = block[
                0, :, part * LEVELS : (part + 1) * LEVELS
            ].astype(F32)
        rows = scratch[...].astype(BF16)
        matrix = v[:, 0].reshape(COV_BANDS * LEVELS, LEVELS)
        total = dot(band_masked(rows, first_total), matrix, ((1,), (0,)))
        out[0, 0] = total.astype(BF16).reshape(rows_dev, 2, LEVELS)

    pl.when(pl.program_id(1) == 0)(lambda: run(own))
    pl.when(pl.program_id(1) == 1)(lambda: run(other))


def vertical_adj(own, other, vertical, info, waves, member, sub, subs, shape, into):
    _, slots, rows_dev, _, _ = shape
    block = (1, 1, rows_dev, 2, LEVELS)
    iblock = (1, rows_dev, 2 * LEVELS)
    column = lambda r, info: (info[0] + r - 2 * info[0] * r) * subs + sub
    in_specs = [
        pl.BlockSpec(iblock, lambda s, r, info, w: (s, 0, 0)),
        pl.BlockSpec(iblock, lambda s, r, info, w: (s, 0, 0)),
        pl.BlockSpec((COV_BANDS, 1, LEVELS, LEVELS), lambda s, r, info, w: (0, column(r, info), 0, 0)),
    ]
    operands = [info, waves, own, other, vertical]
    aliases = {}
    if into is not None:
        in_specs.append(pl.BlockSpec(memory_space=pl.ANY))
        operands.append(into)
        aliases = {5: 0}
    return pl.pallas_call(
        vertical_adj_body,
        grid_spec=pltpu.PrefetchScalarGridSpec(
            num_scalar_prefetch=2,
            grid=(slots, 2),
            in_specs=in_specs,
            out_specs=pl.BlockSpec(block, lambda s, r, info, w: (member, s, 0, 0, column(r, info))),
            scratch_shapes=[pltpu.VMEM((2 * rows_dev, LEVELS), F32)],
        ),
        out_shape=jax.ShapeDtypeStruct(shape, BF16),
        input_output_aliases=aliases,
        compiler_params=params("arbitrary", "arbitrary"),
        cost_estimate=cost(16 * slots * rows_dev * COV_BANDS * LEVELS * LEVELS, 8 * slots * rows_dev * 256),
        name="vertical_adj",
    )(*operands)


def legendre_fwd_body(lo, lx, own, recv, out, scratch):
    slot = pl.program_id(0)
    groups, lats, slots, width = out.shape
    total = dot(lo[0], own[0], ((0,), (0,))) + dot(lx[0], recv[0], ((0,), (0,)))
    for tile in range(width // LANES):
        scratch[tile, pl.ds(slot, groups * lats, stride=slots), :] = total[:, tile * LANES : (tile + 1) * LANES]

    @pl.when(slot == slots - 1)
    def _():
        for group in range(groups):
            for tile in range(width // LANES):
                rows = scratch[tile, group * lats * slots : (group + 1) * lats * slots, :]
                out[group, :, :, tile * LANES : (tile + 1) * LANES] = rows.astype(BF16).reshape(lats, slots, LANES)


def legendre_fwd(leg_own, leg_other, own, recv, groups):
    slots, rows_dev, latitudes = leg_own.shape
    width = own.shape[2]
    lats = latitudes // groups
    row = pl.BlockSpec((1, rows_dev, latitudes), lambda s: (s, 0, 0))
    col = pl.BlockSpec((1, rows_dev, width), lambda s: (s, 0, 0))
    shape = (groups, lats, slots, width)
    return pl.pallas_call(
        legendre_fwd_body,
        grid=(slots,),
        in_specs=[row, row, col, col],
        out_specs=pl.BlockSpec(shape, lambda s: (0, 0, 0, 0)),
        out_shape=jax.ShapeDtypeStruct(shape, BF16),
        scratch_shapes=[pltpu.VMEM((width // LANES, latitudes * slots, LANES), F32)],
        compiler_params=params("arbitrary"),
        cost_estimate=cost(4 * slots * rows_dev * latitudes * width, 8 * slots * rows_dev * width),
        name="legendre_fwd",
    )(leg_own, leg_other, own, recv)


def legendre_adj_body(lo, lx, band, own, send, scratch):
    slot = pl.program_id(0)
    groups, lats, slots, width = band.shape

    @pl.when(slot == 0)
    def _():
        for group in range(groups):
            for tile in range(width // LANES):
                rows = band[group, :, :, tile * LANES : (tile + 1) * LANES].reshape(lats * slots, LANES)
                scratch[tile, group * lats * slots : (group + 1) * lats * slots, :] = rows.astype(F32)

    rows = jnp.concatenate(
        [scratch[tile, pl.ds(slot, groups * lats, stride=slots), :] for tile in range(width // LANES)], axis=1
    ).astype(BF16)
    own[0] = dot(lo[0], rows, ((1,), (0,))).astype(BF16)
    send[0] = dot(lx[0], rows, ((1,), (0,))).astype(BF16)


def legendre_adj(leg_own, leg_other, band_rows):
    slots, rows_dev, latitudes = leg_own.shape
    width = band_rows.shape[3]
    row = pl.BlockSpec((1, rows_dev, latitudes), lambda s: (s, 0, 0))
    col = pl.BlockSpec((1, rows_dev, width), lambda s: (s, 0, 0))
    shape = jax.ShapeDtypeStruct((slots, rows_dev, width), BF16)
    return pl.pallas_call(
        legendre_adj_body,
        grid=(slots,),
        in_specs=[row, row, pl.BlockSpec(band_rows.shape, lambda s: (0, 0, 0, 0))],
        out_specs=[col, col],
        out_shape=[shape, shape],
        scratch_shapes=[pltpu.VMEM((width // LANES, latitudes * slots, LANES), F32)],
        compiler_params=params("arbitrary"),
        cost_estimate=cost(4 * slots * rows_dev * latitudes * width, 8 * slots * rows_dev * width),
        name="legendre_adj",
    )(leg_own, leg_other, band_rows)


def table_body(points, waves, cosine, sine):
    count_i = points[pl.program_id(0)]
    count = jnp.full((1, 1), count_i, jnp.int32).astype(F32)
    inverse = 1.0 / count
    wave = waves[...]
    lon_i = lax.broadcasted_iota(jnp.int32, cosine.shape[1:], 1)
    product = wave * lon_i.astype(F32)
    rest = product - jnp.floor(product * inverse) * count
    rest = jnp.where(rest < 0.0, rest + count, rest)
    rest = jnp.where(rest >= count, rest - count, rest)
    quarters = rest * (4.0 * inverse)
    whole = jnp.floor(quarters + 0.5)
    x = (quarters - whole) * (0.5 * math.pi)
    y = x * x
    s = x * (1.0 + y * (-1.0 / 6 + y * (1.0 / 120 + y * (-1.0 / 5040 + y * (1.0 / 362880)))))
    c = 1.0 + y * (-0.5 + y * (1.0 / 24 + y * (-1.0 / 720 + y * (1.0 / 40320))))
    turn = whole.astype(jnp.int32)
    odd = (turn & 1) != 0
    factor = jnp.where(wave == 0.0, 1.0, 2.0) / math.sqrt(4.0 * WAVES)
    factor = jnp.where(lon_i < count_i, factor, 0.0)
    cos_factor = jnp.where(((turn + 1) & 2) != 0, -factor, factor)
    sin_factor = jnp.where((turn & 2) != 0, factor, -factor)
    cosine[0] = (cos_factor * jnp.where(odd, s, c)).astype(BF16)
    sine[0] = (sin_factor * jnp.where(odd, c, s)).astype(BF16)


def fourier_tables(points, wave_of_slot):
    lats, count = points.shape[0], wave_of_slot.shape[0]
    shape = jax.ShapeDtypeStruct((lats, count, LONGITUDES), BF16)
    block = pl.BlockSpec((1, count, LONGITUDES), lambda t, n: (t, 0, 0))
    return pl.pallas_call(
        table_body,
        grid_spec=pltpu.PrefetchScalarGridSpec(
            num_scalar_prefetch=1,
            grid=(lats,),
            in_specs=[pl.BlockSpec((count, 1), lambda t, n: (0, 0))],
            out_specs=[block, block],
        ),
        out_shape=[shape, shape],
        compiler_params=params("arbitrary"),
        cost_estimate=cost(40 * lats * count * LONGITUDES, 4 * lats * count * LONGITUDES),
        name="fourier_tables",
    )(points, wave_of_slot.astype(F32)[:, None])


def grid_body(by_lat, cosine, sine, scale, weight, *rest):
    increment, adjoint = rest[-2:]
    groups, _, slots, width = by_lat.shape
    half = width // 2
    rows = by_lat[:, 0].reshape(groups * slots, width)
    synthesis = dot(rows[:, :half], cosine[0], ((0,), (0,)))
    synthesis = synthesis + dot(rows[:, half:], sine[0], ((0,), (0,)))
    lat_scale = scale[0]
    inc = (synthesis * lat_scale).astype(BF16)
    increment[0, 0] = inc
    weighted = (inc.astype(F32) * weight[0].astype(F32) * lat_scale).astype(BF16)
    for part, table in ((0, cosine), (1, sine)):
        total = dot(table[0], weighted, ((1,), (1,))).astype(BF16)
        adjoint[:, 0, :, part * half : (part + 1) * half] = total.reshape(groups, slots, half)


def grid_stage(by_lat, tables, lat_scale, obs_weight, member, sub, shape, into):
    groups, lats, slots, width = by_lat.shape
    half = width // 2
    count = groups * slots
    table = pl.BlockSpec((1, count, LONGITUDES), lambda t: (t, 0, 0))
    lat_rows = pl.BlockSpec((groups, 1, slots, width), lambda t: (0, t, 0, 0))
    in_specs = [
        lat_rows,
        table,
        table,
        pl.BlockSpec((1, half, 1), lambda t: (t, sub, 0)),
        pl.BlockSpec((1, half, LONGITUDES), lambda t: (t, sub, 0)),
    ]
    operands = [by_lat, *tables, lat_scale, obs_weight]
    aliases = {}
    if into is not None:
        in_specs.append(pl.BlockSpec(memory_space=pl.ANY))
        operands.append(into)
        aliases = {5: 0}
    return pl.pallas_call(
        grid_body,
        grid=(lats,),
        in_specs=in_specs,
        out_specs=[
            pl.BlockSpec((1, 1, half, LONGITUDES), lambda t: (member, t, sub, 0)),
            lat_rows,
        ],
        out_shape=[jax.ShapeDtypeStruct(shape, BF16), jax.ShapeDtypeStruct(by_lat.shape, BF16)],
        input_output_aliases=aliases,
        compiler_params=params("arbitrary"),
        cost_estimate=cost(4 * lats * count * LONGITUDES * width, 6 * lats * count * LONGITUDES),
        name="grid_stage",
    )(*operands)


def swap(values):
    return lax.ppermute(values, "lev", [(0, 1), (1, 0)])


def exchange(values):
    return lax.all_to_all(values, "wave", split_axis=0, concat_axis=0, tiled=True)


def chunked(control, wave_of_slot, legendre, vertical, points, lat_band, grid_scale, obs_weight):
    members, slots, rows_dev = control.shape[:3]
    groups = legendre.shape[2] // points.shape[0]
    lats, col_dev, _ = obs_weight.shape
    subs = col_dev // LEVELS
    info = lax.axis_index("lev").astype(jnp.int32)[None]
    waves = lax.dynamic_slice_in_dim(wave_of_slot, lax.axis_index("wave") * slots, slots)
    chooser = (
        lat_band[:, None] == jnp.arange(grid_scale.shape[0], dtype=jnp.int32)[None, :]
    ).astype(F32)
    lat_scale = jnp.dot(chooser, grid_scale, precision=lax.Precision.HIGHEST)[:, :, None]
    chunks = [(member, sub) for member in range(members) for sub in range(subs)]

    leg_other = swap(legendre)
    received = []
    for member, sub in chunks:
        own, send = vertical_fwd(control, vertical, info, waves, member, sub, subs)
        received.append((own, swap(send)))
    tables = fourier_tables(points, wave_of_slot)
    increment = gradient = None
    bands = []
    for (member, sub), (own, recv) in zip(chunks, received):
        by_lat = exchange(legendre_fwd(legendre, leg_other, own, recv, groups))
        increment, adjoint = grid_stage(
            by_lat, tables, lat_scale, obs_weight, member, sub, (members, lats, col_dev, LONGITUDES), increment
        )
        bands.append(adjoint)
    for (member, sub), adjoint in zip(chunks, bands):
        own, send = legendre_adj(legendre, leg_other, exchange(adjoint))
        gradient = vertical_adj(
            own, swap(send), vertical, info, waves, member, sub, subs, control.shape, gradient
        )
    return (increment, gradient)


def fourier_table(wave_ids, lat_points):
    lon_index = jnp.arange(LONGITUDES, dtype=jnp.int32)
    remainder = wave_ids[None, :, None] * lon_index[None, None, :] % lat_points[:, None, None]
    angles = (
        2.0
        * math.pi
        * remainder.astype(jnp.float32)
        / lat_points.astype(jnp.float32)[:, None, None]
    )
    factor = jnp.where(wave_ids == 0, 1.0, 2.0).astype(jnp.float32) / math.sqrt(4.0 * WAVES)
    inside = lon_index[None, None, :] < lat_points[:, None, None]
    cosine = jnp.where(inside, factor[None, :, None] * jnp.cos(angles), 0.0)
    sine = jnp.where(inside, -factor[None, :, None] * jnp.sin(angles), 0.0)
    return jnp.stack([cosine, sine], axis=2).astype(jnp.bfloat16)


def vertical_apply(field, vertical, live_rows, band_of, forward):
    members, slots, rows_dev = (field.shape[0], field.shape[1], field.shape[2])
    shaped = field.reshape(members, slots, rows_dev, 2, VARIABLES, LEVELS)
    form = "eskpam,alm->eskpal" if forward else "eskpal,alm->eskpam"
    summed = jnp.zeros(shaped.shape, jnp.float32)
    for index_band in range(COV_BANDS):
        partial_value = jnp.einsum(
            form, shaped, vertical[index_band], preferred_element_type=jnp.float32
        )
        chosen = live_rows & (band_of == index_band)
        summed = summed + jnp.where(chosen[None, :, :, None, None, None], partial_value, 0.0)
    return summed.reshape(field.shape).astype(jnp.bfloat16)


def to_bands(values):
    return lax.all_to_all(values, "wave", split_axis=2, concat_axis=1, tiled=True)


def shards(control, wave_of_slot, legendre, vertical, points, lat_band, grid_scale, obs_weight):
    members, slots, rows_dev = (control.shape[0], control.shape[1], control.shape[2])
    slot_start = lax.axis_index("wave") * slots
    row_start = lax.axis_index("lev") * rows_dev
    own_waves = lax.dynamic_slice_in_dim(wave_of_slot, slot_start, slots)
    row_index = row_start + jnp.arange(rows_dev, dtype=jnp.int32)
    totals_n = own_waves[:, None] + row_index[None, :]
    live_rows = totals_n <= WAVES - 1
    band_of = jnp.minimum(totals_n * COV_BANDS // WAVES, COV_BANDS - 1)
    spectral = vertical_apply(control, vertical, live_rows, band_of, True)
    columns = lax.all_to_all(spectral, "lev", split_axis=4, concat_axis=2, tiled=True)
    col_dev = columns.shape[4]
    width = 2 * col_dev
    all_rows = columns.shape[2]
    columns = columns.reshape(members, slots, all_rows, width)
    coeffs = jnp.einsum(
        "skt,eskq->estq",
        lax.all_gather(legendre, "lev", axis=1, tiled=True),
        columns,
        preferred_element_type=jnp.float32,
    )
    coeffs = coeffs.astype(jnp.bfloat16)
    by_lat = to_bands(coeffs)
    wave_count = by_lat.shape[1]
    lat_dev = by_lat.shape[2]
    by_lat = by_lat.reshape(members, wave_count, lat_dev, 2, col_dev)
    fourier = fourier_table(wave_of_slot, points)
    synthesis = jnp.einsum("tspj,estpc->etcj", fourier, by_lat, preferred_element_type=jnp.float32)
    chooser = (
        lat_band[:, None] == jnp.arange(grid_scale.shape[0], dtype=jnp.int32)[None, :]
    ).astype(jnp.float32)
    lat_scale = jnp.dot(chooser, grid_scale, precision=lax.Precision.HIGHEST)
    increment = (synthesis * lat_scale[None, :, :, None]).astype(jnp.bfloat16)
    weighted = (
        increment.astype(jnp.float32) * obs_weight.astype(jnp.float32) * lat_scale[None, :, :, None]
    ).astype(jnp.bfloat16)
    adjoint_fourier = jnp.einsum(
        "tspj,etcj->etspc", fourier, weighted, preferred_element_type=jnp.float32
    )
    adjoint_fourier = adjoint_fourier.astype(jnp.bfloat16).reshape(
        members, lat_dev, wave_count, width
    )
    band_rows = to_bands(adjoint_fourier)
    adjoint_coeffs = jnp.einsum(
        "skt,etsq->eskq",
        lax.all_gather(legendre, "lev", axis=1, tiled=True),
        band_rows,
        preferred_element_type=jnp.float32,
    )
    adjoint_coeffs = adjoint_coeffs.astype(jnp.bfloat16).reshape(
        members, slots, all_rows, 2, col_dev
    )
    rows_back = lax.all_to_all(adjoint_coeffs, "lev", split_axis=2, concat_axis=4, tiled=True)
    gradient = vertical_apply(rows_back, vertical, live_rows, band_of, False)
    return (increment, gradient)


def solution(mesh):
    in_specs = (
        P(None, "wave", "lev", None, None),
        P(),
        P("wave", "lev", None),
        P(),
        P("wave"),
        P("wave"),
        P(None, "lev"),
        P("wave", "lev", None),
    )
    out_specs = (P(None, "wave", "lev", None), P(None, "wave", "lev", None, None))

    def body(control, *rest):
        levs = mesh.shape["lev"]
        slots, rows_dev = control.shape[1:3]
        whole_blocks = slots % 16 == 0 and rows_dev % 16 == 0 and rest[3].shape[0] % 16 == 0
        if levs == 2 and control.shape[4] % (levs * LEVELS) == 0 and whole_blocks:
            return chunked(control, *rest)
        return shards(control, *rest)

    return jax.shard_map(body, mesh=mesh, in_specs=in_specs, out_specs=out_specs, check_vma=False)
```

```python
import functools
import math

import jax
import jax.numpy as jnp
from jax import lax
from jax.experimental import pallas as pl
from jax.experimental.pallas import tpu as pltpu
from jax.sharding import PartitionSpec as P


WAVES = 256
LONGITUDES = 512
LEVELS = 128
VARIABLES = 4
COV_BANDS = 4
LANES = 128
STEP = 4

BF16 = jnp.bfloat16
F32 = jnp.float32


def params(*semantics):
    return pltpu.CompilerParams(dimension_semantics=semantics, vmem_limit_bytes=56 << 20)


def cost(flops, nbytes):
    return pl.CostEstimate(flops=int(flops), bytes_accessed=int(nbytes), transcendentals=0)


def dot(a, b, contract):
    return lax.dot_general(a, b, (contract, ((), ())), preferred_element_type=F32)


def band_masks(count, first_total):
    row_total = first_total + (lax.broadcasted_iota(jnp.int32, (count, LEVELS), 0) >> 1)
    width = WAVES // COV_BANDS
    masks = []
    for band in range(COV_BANDS):
        inside = (row_total >= band * width) & (row_total < (band + 1) * width)
        masks.append(jnp.where(inside, 1.0, 0.0).astype(BF16))
    return masks


def band_rows_of(rows, first_total):
    return jnp.concatenate([rows * mask for mask in band_masks(rows.shape[0], first_total)], axis=1)


def vertical_fwd_body(first_slot, info, waves, x, v, out, scratch):
    step, rows_dev = out.shape[:2]
    matrix = jnp.concatenate([v[band, 0] for band in range(COV_BANDS)], axis=1)

    @pl.loop(0, step)
    def _(i):
        slot = first_slot + pl.program_id(0) * step + i
        first_total = waves[slot] + info[0] * rows_dev
        rows = x[0, i].reshape(2 * rows_dev, LEVELS)
        scratch[...] = dot(band_rows_of(rows, first_total), matrix, ((1,), (1,)))
        for part in range(2):
            out[i, :, part * LEVELS : (part + 1) * LEVELS] = scratch[
                pl.ds(part, rows_dev, stride=2), :
            ].astype(BF16)


def column_of(info, sub, subs, other):
    lev = (1 - info[0]) if other else info[0]
    return lev * subs + sub


def vertical_fwd(control, vertical, info, waves, where, first_slot, slots):
    member, sub, subs, other = where
    rows_dev = control.shape[2]
    step = STEP if slots % STEP == 0 else 1
    first = first_slot // step
    column = lambda info: column_of(info, sub, subs, other)
    return pl.pallas_call(
        functools.partial(vertical_fwd_body, first_slot),
        grid_spec=pltpu.PrefetchScalarGridSpec(
            num_scalar_prefetch=2,
            grid=(slots // step,),
            in_specs=[
                pl.BlockSpec(
                    (1, step, rows_dev, 2, LEVELS), lambda s, info, w: (member, first + s, 0, 0, column(info))
                ),
                pl.BlockSpec((COV_BANDS, 1, LEVELS, LEVELS), lambda s, info, w: (0, column(info), 0, 0)),
            ],
            out_specs=pl.BlockSpec((step, rows_dev, 2 * LEVELS), lambda s, info, w: (s, 0, 0)),
            scratch_shapes=[pltpu.VMEM((2 * rows_dev, LEVELS), F32)],
        ),
        out_shape=jax.ShapeDtypeStruct((slots, rows_dev, 2 * LEVELS), BF16),
        compiler_params=params("arbitrary"),
        cost_estimate=cost(64 * slots * rows_dev * COV_BANDS * LEVELS * LEVELS, 8 * slots * rows_dev * 256),
        name="vertical_fwd",
    )(info, waves, control, vertical)


def vertical_adj_body(first_slot, info, waves, block, v, *rest):
    out, scratch = rest[-2:]
    step, rows_dev = block.shape[:2]
    matrix = v[:, 0].reshape(COV_BANDS * LEVELS, LEVELS)

    @pl.loop(0, step)
    def _(i):
        slot = first_slot + pl.program_id(0) * step + i
        first_total = waves[slot] + info[0] * rows_dev
        for part in range(2):
            scratch[pl.ds(part, rows_dev, stride=2), :] = block[
                i, :, part * LEVELS : (part + 1) * LEVELS
            ].astype(F32)
        rows = scratch[...].astype(BF16)
        total = dot(band_rows_of(rows, first_total), matrix, ((1,), (0,)))
        out[0, i] = total.astype(BF16).reshape(rows_dev, 2, LEVELS)


def vertical_adj(block, vertical, info, waves, where, first_slot, shape, into):
    member, sub, subs, other = where
    slots, rows_dev, width = block.shape
    step = STEP if slots % STEP == 0 else 1
    first = first_slot // step
    column = lambda info: column_of(info, sub, subs, other)
    in_specs = [
        pl.BlockSpec((step, rows_dev, width), lambda s, info, w: (s, 0, 0)),
        pl.BlockSpec((COV_BANDS, 1, LEVELS, LEVELS), lambda s, info, w: (0, column(info), 0, 0)),
    ]
    operands = [info, waves, block, vertical]
    aliases = {}
    if into is not None:
        in_specs.append(pl.BlockSpec(memory_space=pl.ANY))
        operands.append(into)
        aliases = {4: 0}
    return pl.pallas_call(
        functools.partial(vertical_adj_body, first_slot),
        grid_spec=pltpu.PrefetchScalarGridSpec(
            num_scalar_prefetch=2,
            grid=(slots // step,),
            in_specs=in_specs,
            out_specs=pl.BlockSpec(
                (1, step, rows_dev, 2, LEVELS), lambda s, info, w: (member, first + s, 0, 0, column(info))
            ),
            scratch_shapes=[pltpu.VMEM((2 * rows_dev, LEVELS), F32)],
        ),
        out_shape=jax.ShapeDtypeStruct(shape, BF16),
        input_output_aliases=aliases,
        compiler_params=params("arbitrary"),
        cost_estimate=cost(64 * slots * rows_dev * COV_BANDS * LEVELS * LEVELS, 8 * slots * rows_dev * 256),
        name="vertical_adj",
    )(*operands)


def legendre_fwd_body(lo, lx, own, recv, out, scratch):
    groups, lats, slots, width = out.shape
    step = own.shape[0]
    for i in range(step):
        slot = pl.program_id(0) * step + i
        total = dot(lo[i], own[i], ((0,), (0,))) + dot(lx[i], recv[i], ((0,), (0,)))
        for tile in range(width // LANES):
            scratch[tile, pl.ds(slot, groups * lats, stride=slots), :] = total[:, tile * LANES : (tile + 1) * LANES]

    @pl.when(pl.program_id(0) == slots // step - 1)
    def _():
        @pl.loop(0, groups)
        def _(group):
            start = pl.multiple_of(group * lats * slots, lats * slots)
            for tile in range(width // LANES):
                rows = scratch[tile, pl.ds(start, lats * slots), :]
                out[group, :, :, tile * LANES : (tile + 1) * LANES] = rows.astype(BF16).reshape(lats, slots, LANES)


def legendre_fwd(leg_own, leg_other, own, recv, groups, first_slot):
    slots, rows_dev, width = own.shape
    latitudes = leg_own.shape[2]
    step = STEP if slots % STEP == 0 else 1
    first = first_slot // step
    lats = latitudes // groups
    row = pl.BlockSpec((step, rows_dev, latitudes), lambda s: (first + s, 0, 0))
    other_row = pl.BlockSpec((step, rows_dev, latitudes), lambda s: (s, 0, 0))
    col = pl.BlockSpec((step, rows_dev, width), lambda s: (s, 0, 0))
    shape = (groups, lats, slots, width)
    return pl.pallas_call(
        legendre_fwd_body,
        grid=(slots // step,),
        in_specs=[row, other_row, col, col],
        out_specs=pl.BlockSpec(shape, lambda s: (0, 0, 0, 0)),
        out_shape=jax.ShapeDtypeStruct(shape, BF16),
        scratch_shapes=[pltpu.VMEM((width // LANES, latitudes * slots, LANES), F32)],
        compiler_params=params("arbitrary"),
        cost_estimate=cost(16 * slots * rows_dev * latitudes * width, 8 * slots * rows_dev * width),
        name="legendre_fwd",
    )(leg_own, leg_other, own, recv)


def legendre_adj_body(lo, lx, band, own, send, scratch):
    groups, lats, slots, width = band.shape
    step = own.shape[0]

    @pl.when(pl.program_id(0) == 0)
    def _():
        @pl.loop(0, groups)
        def _(group):
            start = pl.multiple_of(group * lats * slots, lats * slots)
            for tile in range(width // LANES):
                rows = band[group, :, :, tile * LANES : (tile + 1) * LANES].reshape(lats * slots, LANES)
                scratch[tile, pl.ds(start, lats * slots), :] = rows.astype(F32)

    for i in range(step):
        slot = pl.program_id(0) * step + i
        rows = jnp.concatenate(
            [scratch[tile, pl.ds(slot, groups * lats, stride=slots), :] for tile in range(width // LANES)], axis=1
        ).astype(BF16)
        own[i] = dot(lo[i], rows, ((1,), (0,))).astype(BF16)
        send[i] = dot(lx[i], rows, ((1,), (0,))).astype(BF16)


def legendre_adj(leg_own, leg_other, band_rows, first_slot):
    _, rows_dev, latitudes = leg_own.shape
    slots, width = band_rows.shape[2:]
    step = STEP if slots % STEP == 0 else 1
    first = first_slot // step
    row = pl.BlockSpec((step, rows_dev, latitudes), lambda s: (first + s, 0, 0))
    other_row = pl.BlockSpec((step, rows_dev, latitudes), lambda s: (s, 0, 0))
    col = pl.BlockSpec((step, rows_dev, width), lambda s: (s, 0, 0))
    shape = jax.ShapeDtypeStruct((slots, rows_dev, width), BF16)
    return pl.pallas_call(
        legendre_adj_body,
        grid=(slots // step,),
        in_specs=[row, other_row, pl.BlockSpec(band_rows.shape, lambda s: (0, 0, 0, 0))],
        out_specs=[col, col],
        out_shape=[shape, shape],
        scratch_shapes=[pltpu.VMEM((width // LANES, latitudes * slots, LANES), F32)],
        compiler_params=params("arbitrary"),
        cost_estimate=cost(16 * slots * rows_dev * latitudes * width, 8 * slots * rows_dev * width),
        name="legendre_adj",
    )(leg_own, leg_other, band_rows)


def table_body(points, waves, cosine, sine):
    count_i = points[pl.program_id(0)]
    count = jnp.full((1, 1), count_i, jnp.int32).astype(F32)
    inverse = 1.0 / count
    wave = waves[...]
    lon_i = lax.broadcasted_iota(jnp.int32, cosine.shape[1:], 1)
    product = wave * lon_i.astype(F32)
    rest = product - jnp.floor(product * inverse) * count
    rest = jnp.where(rest < 0.0, rest + count, rest)
    rest = jnp.where(rest >= count, rest - count, rest)
    quarters = rest * (4.0 * inverse)
    whole = jnp.floor(quarters + 0.5)
    x = (quarters - whole) * (0.5 * math.pi)
    y = x * x
    s = x * (1.0 + y * (-1.0 / 6 + y * (1.0 / 120 + y * (-1.0 / 5040 + y * (1.0 / 362880)))))
    c = 1.0 + y * (-0.5 + y * (1.0 / 24 + y * (-1.0 / 720 + y * (1.0 / 40320))))
    turn = whole.astype(jnp.int32)
    odd = (turn & 1) != 0
    factor = jnp.where(wave == 0.0, 1.0, 2.0) / math.sqrt(4.0 * WAVES)
    factor = jnp.where(lon_i < count_i, factor, 0.0)
    cos_factor = jnp.where(((turn + 1) & 2) != 0, -factor, factor)
    sin_factor = jnp.where((turn & 2) != 0, factor, -factor)
    cosine[0] = (cos_factor * jnp.where(odd, s, c)).astype(BF16)
    sine[0] = (sin_factor * jnp.where(odd, c, s)).astype(BF16)


def fourier_tables(points, wave_of_slot):
    lats, count = points.shape[0], wave_of_slot.shape[0]
    shape = jax.ShapeDtypeStruct((lats, count, LONGITUDES), BF16)
    block = pl.BlockSpec((1, count, LONGITUDES), lambda t, n: (t, 0, 0))
    return pl.pallas_call(
        table_body,
        grid_spec=pltpu.PrefetchScalarGridSpec(
            num_scalar_prefetch=1,
            grid=(lats,),
            in_specs=[pl.BlockSpec((count, 1), lambda t, n: (0, 0))],
            out_specs=[block, block],
        ),
        out_shape=[shape, shape],
        compiler_params=params("arbitrary"),
        cost_estimate=cost(40 * lats * count * LONGITUDES, 4 * lats * count * LONGITUDES),
        name="fourier_tables",
    )(points, wave_of_slot.astype(F32)[:, None])


def grid_body(by_lat, cosine, sine, scale, weight, *rest):
    increment, adjoint = rest[-2:]
    groups, _, slots, width = by_lat.shape
    half = width // 2
    rows = by_lat[:, 0].reshape(groups * slots, width)
    synthesis = dot(rows[:, :half], cosine[0], ((0,), (0,)))
    synthesis = synthesis + dot(rows[:, half:], sine[0], ((0,), (0,)))
    lat_scale = scale[0]
    inc = (synthesis * lat_scale).astype(BF16)
    increment[0, 0] = inc
    weighted = (inc.astype(F32) * weight[0].astype(F32) * lat_scale).astype(BF16)
    for part, table in ((0, cosine), (1, sine)):
        total = dot(table[0], weighted, ((1,), (1,))).astype(BF16)
        adjoint[:, 0, :, part * half : (part + 1) * half] = total.reshape(groups, slots, half)


def grid_stage(by_lat, tables, lat_scale, obs_weight, member, sub, shape, into):
    groups, lats, slots, width = by_lat.shape
    half = width // 2
    count = groups * slots
    table = pl.BlockSpec((1, count, LONGITUDES), lambda t: (t, 0, 0))
    lat_rows = pl.BlockSpec((groups, 1, slots, width), lambda t: (0, t, 0, 0))
    in_specs = [
        lat_rows,
        table,
        table,
        pl.BlockSpec((1, half, 1), lambda t: (t, sub, 0)),
        pl.BlockSpec((1, half, LONGITUDES), lambda t: (t, sub, 0)),
    ]
    operands = [by_lat, *tables, lat_scale, obs_weight]
    aliases = {}
    if into is not None:
        in_specs.append(pl.BlockSpec(memory_space=pl.ANY))
        operands.append(into)
        aliases = {5: 0}
    return pl.pallas_call(
        grid_body,
        grid=(lats,),
        in_specs=in_specs,
        out_specs=[
            pl.BlockSpec((1, 1, half, LONGITUDES), lambda t: (member, t, sub, 0)),
            lat_rows,
        ],
        out_shape=[jax.ShapeDtypeStruct(shape, BF16), jax.ShapeDtypeStruct(by_lat.shape, BF16)],
        input_output_aliases=aliases,
        compiler_params=params("arbitrary"),
        cost_estimate=cost(4 * lats * count * LONGITUDES * width, 6 * lats * count * LONGITUDES),
        name="grid_stage",
    )(*operands)


def swap(values):
    return lax.ppermute(values, "lev", [(0, 1), (1, 0)])


def exchange(values):
    return lax.all_to_all(values, "wave", split_axis=0, concat_axis=0, tiled=True)


def chunked(control, wave_of_slot, legendre, vertical, points, lat_band, grid_scale, obs_weight):
    members, slots, _ = control.shape[:3]
    groups = legendre.shape[2] // points.shape[0]
    lats, col_dev, _ = obs_weight.shape
    subs = col_dev // LEVELS
    half = slots // 2
    grid_shape = (members, lats, col_dev, LONGITUDES)
    info = lax.axis_index("lev").astype(jnp.int32)[None]
    waves = lax.dynamic_slice_in_dim(wave_of_slot, lax.axis_index("wave") * slots, slots)
    chooser = (
        lat_band[:, None] == jnp.arange(grid_scale.shape[0], dtype=jnp.int32)[None, :]
    ).astype(F32)
    lat_scale = jnp.dot(chooser, grid_scale, precision=lax.Precision.HIGHEST)[:, :, None]
    chunks = [(member, sub) for member in range(members) for sub in range(subs)]
    last = len(chunks) - 1
    whole = [(q, 0, slots) for q in range(len(chunks))]
    units_out = [(0, 0, half), (0, half, half)] + whole[1:]
    units_back = whole[:-1] + [(last, 0, half), (last, half, half)]

    leg_parts = []
    for first in (0, half):
        leg_parts.append(swap(legendre[first : first + half]))
    fields = []
    for q, first, count in units_out:
        member, sub = chunks[q]
        sent = vertical_fwd(control, vertical, info, waves, (member, sub, subs, True), first, count)
        recv = swap(sent)
        own = vertical_fwd(control, vertical, info, waves, (member, sub, subs, False), first, count)
        fields.append((own, recv))
    tables = fourier_tables(points, wave_of_slot)
    leg_other = jnp.concatenate(leg_parts, axis=0)

    arrived = [[] for _ in chunks]
    for (q, first, count), (own, recv) in zip(units_out, fields):
        partner = leg_other if count == slots else leg_parts[first // half]
        coeffs = legendre_fwd(legendre, partner, own, recv, groups, first)
        arrived[q].append(exchange(coeffs))
    increment = gradient = None
    adjoints = []
    for q, (member, sub) in enumerate(chunks):
        by_lat = arrived[q][0] if len(arrived[q]) == 1 else jnp.concatenate(arrived[q], axis=2)
        increment, adjoint = grid_stage(
            by_lat, tables, lat_scale, obs_weight, member, sub, grid_shape, increment
        )
        adjoints.append(adjoint)
    for q, first, count in units_back:
        member, sub = chunks[q]
        partner = leg_other if count == slots else leg_parts[first // half]
        band_rows = exchange(adjoints[q] if count == slots else adjoints[q][:, :, first : first + count])
        own, sent = legendre_adj(legendre, partner, band_rows, first)
        recv = swap(sent)
        for block, other in ((own, False), (recv, True)):
            gradient = vertical_adj(
                block, vertical, info, waves, (member, sub, subs, other), first, control.shape, gradient
            )
    return (increment, gradient)


def fourier_table(wave_ids, lat_points):
    lon_index = jnp.arange(LONGITUDES, dtype=jnp.int32)
    remainder = wave_ids[None, :, None] * lon_index[None, None, :] % lat_points[:, None, None]
    angles = (
        2.0
        * math.pi
        * remainder.astype(jnp.float32)
        / lat_points.astype(jnp.float32)[:, None, None]
    )
    factor = jnp.where(wave_ids == 0, 1.0, 2.0).astype(jnp.float32) / math.sqrt(4.0 * WAVES)
    inside = lon_index[None, None, :] < lat_points[:, None, None]
    cosine = jnp.where(inside, factor[None, :, None] * jnp.cos(angles), 0.0)
    sine = jnp.where(inside, -factor[None, :, None] * jnp.sin(angles), 0.0)
    return jnp.stack([cosine, sine], axis=2).astype(jnp.bfloat16)


def vertical_apply(field, vertical, live_rows, band_of, forward):
    members, slots, rows_dev = (field.shape[0], field.shape[1], field.shape[2])
    shaped = field.reshape(members, slots, rows_dev, 2, VARIABLES, LEVELS)
    form = "eskpam,alm->eskpal" if forward else "eskpal,alm->eskpam"
    summed = jnp.zeros(shaped.shape, jnp.float32)
    for index_band in range(COV_BANDS):
        partial_value = jnp.einsum(
            form, shaped, vertical[index_band], preferred_element_type=jnp.float32
        )
        chosen = live_rows & (band_of == index_band)
        summed = summed + jnp.where(chosen[None, :, :, None, None, None], partial_value, 0.0)
    return summed.reshape(field.shape).astype(jnp.bfloat16)


def to_bands(values):
    return lax.all_to_all(values, "wave", split_axis=2, concat_axis=1, tiled=True)


def shards(control, wave_of_slot, legendre, vertical, points, lat_band, grid_scale, obs_weight):
    members, slots, rows_dev = (control.shape[0], control.shape[1], control.shape[2])
    slot_start = lax.axis_index("wave") * slots
    row_start = lax.axis_index("lev") * rows_dev
    own_waves = lax.dynamic_slice_in_dim(wave_of_slot, slot_start, slots)
    row_index = row_start + jnp.arange(rows_dev, dtype=jnp.int32)
    totals_n = own_waves[:, None] + row_index[None, :]
    live_rows = totals_n <= WAVES - 1
    band_of = jnp.minimum(totals_n * COV_BANDS // WAVES, COV_BANDS - 1)
    spectral = vertical_apply(control, vertical, live_rows, band_of, True)
    columns = lax.all_to_all(spectral, "lev", split_axis=4, concat_axis=2, tiled=True)
    col_dev = columns.shape[4]
    width = 2 * col_dev
    all_rows = columns.shape[2]
    columns = columns.reshape(members, slots, all_rows, width)
    coeffs = jnp.einsum(
        "skt,eskq->estq",
        lax.all_gather(legendre, "lev", axis=1, tiled=True),
        columns,
        preferred_element_type=jnp.float32,
    )
    coeffs = coeffs.astype(jnp.bfloat16)
    by_lat = to_bands(coeffs)
    wave_count = by_lat.shape[1]
    lat_dev = by_lat.shape[2]
    by_lat = by_lat.reshape(members, wave_count, lat_dev, 2, col_dev)
    fourier = fourier_table(wave_of_slot, points)
    synthesis = jnp.einsum("tspj,estpc->etcj", fourier, by_lat, preferred_element_type=jnp.float32)
    chooser = (
        lat_band[:, None] == jnp.arange(grid_scale.shape[0], dtype=jnp.int32)[None, :]
    ).astype(jnp.float32)
    lat_scale = jnp.dot(chooser, grid_scale, precision=lax.Precision.HIGHEST)
    increment = (synthesis * lat_scale[None, :, :, None]).astype(jnp.bfloat16)
    weighted = (
        increment.astype(jnp.float32) * obs_weight.astype(jnp.float32) * lat_scale[None, :, :, None]
    ).astype(jnp.bfloat16)
    adjoint_fourier = jnp.einsum(
        "tspj,etcj->etspc", fourier, weighted, preferred_element_type=jnp.float32
    )
    adjoint_fourier = adjoint_fourier.astype(jnp.bfloat16).reshape(
        members, lat_dev, wave_count, width
    )
    band_rows = to_bands(adjoint_fourier)
    adjoint_coeffs = jnp.einsum(
        "skt,etsq->eskq",
        lax.all_gather(legendre, "lev", axis=1, tiled=True),
        band_rows,
        preferred_element_type=jnp.float32,
    )
    adjoint_coeffs = adjoint_coeffs.astype(jnp.bfloat16).reshape(
        members, slots, all_rows, 2, col_dev
    )
    rows_back = lax.all_to_all(adjoint_coeffs, "lev", split_axis=2, concat_axis=4, tiled=True)
    gradient = vertical_apply(rows_back, vertical, live_rows, band_of, False)
    return (increment, gradient)


def solution(mesh):
    in_specs = (
        P(None, "wave", "lev", None, None),
        P(),
        P("wave", "lev", None),
        P(),
        P("wave"),
        P("wave"),
        P(None, "lev"),
        P("wave", "lev", None),
    )
    out_specs = (P(None, "wave", "lev", None), P(None, "wave", "lev", None, None))

    def body(control, *rest):
        levs = mesh.shape["lev"]
        slots, rows_dev = control.shape[1:3]
        whole_blocks = slots % 16 == 0 and rows_dev % 16 == 0 and rest[3].shape[0] % 16 == 0
        if levs == 2 and control.shape[4] % (levs * LEVELS) == 0 and whole_blocks:
            return chunked(control, *rest)
        return shards(control, *rest)

    return jax.shard_map(body, mesh=mesh, in_specs=in_specs, out_specs=out_specs, check_vma=False)
```

```python
import functools
import math

import jax
import jax.numpy as jnp
from jax import lax
from jax.experimental import pallas as pl
from jax.experimental.pallas import tpu as pltpu
from jax.sharding import PartitionSpec as P


WAVES = 256
LONGITUDES = 512
LEVELS = 128
VARIABLES = 4
COV_BANDS = 4
LANES = 128
STEP = 4
NEAR = 4


BF16 = jnp.bfloat16
F32 = jnp.float32


def params(*semantics):
    return pltpu.CompilerParams(dimension_semantics=semantics, vmem_limit_bytes=56 << 20)


def cost(flops, nbytes):
    return pl.CostEstimate(flops=int(flops), bytes_accessed=int(nbytes), transcendentals=0)


def dot(a, b, contract):
    return lax.dot_general(a, b, (contract, ((), ())), preferred_element_type=F32)


def band_masks(count, first_total):
    row_total = first_total + (lax.broadcasted_iota(jnp.int32, (count, LEVELS), 0) >> 1)
    width = WAVES // COV_BANDS
    masks = []
    for band in range(COV_BANDS):
        inside = (row_total >= band * width) & (row_total < (band + 1) * width)
        masks.append(jnp.where(inside, 1.0, 0.0).astype(BF16))
    return masks


def band_rows_of(rows, first_total):
    return jnp.concatenate([rows * mask for mask in band_masks(rows.shape[0], first_total)], axis=1)


def vertical_fwd_body(first_slot, info, waves, x, v, out, scratch):
    step, rows_dev = out.shape[:2]
    matrix = jnp.concatenate([v[band, 0] for band in range(COV_BANDS)], axis=1)

    @pl.loop(0, step)
    def _(i):
        slot = first_slot + pl.program_id(0) * step + i
        first_total = waves[slot] + info[0] * rows_dev
        rows = x[0, i].reshape(2 * rows_dev, LEVELS)
        scratch[...] = dot(band_rows_of(rows, first_total), matrix, ((1,), (1,)))
        for part in range(2):
            out[i, :, part * LEVELS : (part + 1) * LEVELS] = scratch[
                pl.ds(part, rows_dev, stride=2), :
            ].astype(BF16)


def column_of(info, sub, subs, other):
    lev = (1 - info[0]) if other else info[0]
    return lev * subs + sub


def vertical_fwd(control, vertical, info, waves, where, first_slot, slots):
    member, sub, subs, other = where
    rows_dev = control.shape[2]
    step = STEP if slots % STEP == 0 else 1
    first = first_slot // step
    column = lambda info: column_of(info, sub, subs, other)
    return pl.pallas_call(
        functools.partial(vertical_fwd_body, first_slot),
        grid_spec=pltpu.PrefetchScalarGridSpec(
            num_scalar_prefetch=2,
            grid=(slots // step,),
            in_specs=[
                pl.BlockSpec(
                    (1, step, rows_dev, 2, LEVELS), lambda s, info, w: (member, first + s, 0, 0, column(info))
                ),
                pl.BlockSpec((COV_BANDS, 1, LEVELS, LEVELS), lambda s, info, w: (0, column(info), 0, 0)),
            ],
            out_specs=pl.BlockSpec((step, rows_dev, 2 * LEVELS), lambda s, info, w: (s, 0, 0)),
            scratch_shapes=[pltpu.VMEM((2 * rows_dev, LEVELS), F32)],
        ),
        out_shape=jax.ShapeDtypeStruct((slots, rows_dev, 2 * LEVELS), BF16),
        compiler_params=params("arbitrary"),
        cost_estimate=cost(64 * slots * rows_dev * COV_BANDS * LEVELS * LEVELS, 8 * slots * rows_dev * 256),
        name="vertical_fwd",
    )(info, waves, control, vertical)


def vertical_adj_body(first_slot, info, waves, block, v, *rest):
    out, scratch = rest[-2:]
    step, rows_dev = block.shape[:2]
    matrix = v[:, 0].reshape(COV_BANDS * LEVELS, LEVELS)

    @pl.loop(0, step)
    def _(i):
        slot = first_slot + pl.program_id(0) * step + i
        first_total = waves[slot] + info[0] * rows_dev
        for part in range(2):
            scratch[pl.ds(part, rows_dev, stride=2), :] = block[
                i, :, part * LEVELS : (part + 1) * LEVELS
            ].astype(F32)
        rows = scratch[...].astype(BF16)
        total = dot(band_rows_of(rows, first_total), matrix, ((1,), (0,)))
        out[0, i] = total.astype(BF16).reshape(rows_dev, 2, LEVELS)


def vertical_adj(block, vertical, info, waves, where, first_slot, shape, into):
    member, sub, subs, other = where
    slots, rows_dev, width = block.shape
    step = STEP if slots % STEP == 0 else 1
    first = first_slot // step
    column = lambda info: column_of(info, sub, subs, other)
    in_specs = [
        pl.BlockSpec((step, rows_dev, width), lambda s, info, w: (s, 0, 0)),
        pl.BlockSpec((COV_BANDS, 1, LEVELS, LEVELS), lambda s, info, w: (0, column(info), 0, 0)),
    ]
    operands = [info, waves, block, vertical]
    aliases = {}
    if into is not None:
        in_specs.append(pl.BlockSpec(memory_space=pl.ANY))
        operands.append(into)
        aliases = {4: 0}
    return pl.pallas_call(
        functools.partial(vertical_adj_body, first_slot),
        grid_spec=pltpu.PrefetchScalarGridSpec(
            num_scalar_prefetch=2,
            grid=(slots // step,),
            in_specs=in_specs,
            out_specs=pl.BlockSpec(
                (1, step, rows_dev, 2, LEVELS), lambda s, info, w: (member, first + s, 0, 0, column(info))
            ),
            scratch_shapes=[pltpu.VMEM((2 * rows_dev, LEVELS), F32)],
        ),
        out_shape=jax.ShapeDtypeStruct(shape, BF16),
        input_output_aliases=aliases,
        compiler_params=params("arbitrary"),
        cost_estimate=cost(64 * slots * rows_dev * COV_BANDS * LEVELS * LEVELS, 8 * slots * rows_dev * 256),
        name="vertical_adj",
    )(*operands)


def legendre_fwd_body(info, lo, lx, own, recv, *rest):
    outs, scratch = rest[:-1], rest[-1]
    inner, lats, slots, width = outs[0].shape
    far = len(outs)
    step = own.shape[0]
    for i in range(step):
        slot = pl.program_id(0) * step + i
        total = dot(lo[i], own[i], ((0,), (0,))) + dot(lx[i], recv[i], ((0,), (0,)))
        for tile in range(width // LANES):
            scratch[tile, pl.ds(slot, far * inner * lats, stride=slots), :] = total[
                :, tile * LANES : (tile + 1) * LANES
            ]

    @pl.when(pl.program_id(0) == slots // step - 1)
    def _():
        for shift, out in enumerate(outs):
            base = (info[1] + shift) % far * inner

            @pl.loop(0, inner)
            def _(near):
                start = pl.multiple_of((base + near) * lats * slots, lats * slots)
                for tile in range(width // LANES):
                    rows = scratch[tile, pl.ds(start, lats * slots), :]
                    out[near, :, :, tile * LANES : (tile + 1) * LANES] = rows.astype(BF16).reshape(
                        lats, slots, LANES
                    )


def legendre_fwd(leg_own, leg_other, own, recv, info, far, inner, first_slot):
    slots, rows_dev, width = own.shape
    latitudes = leg_own.shape[2]
    step = STEP if slots % STEP == 0 else 1
    first = first_slot // step
    lats = latitudes // (far * inner)
    shape = (inner, lats, slots, width)
    return pl.pallas_call(
        legendre_fwd_body,
        grid_spec=pltpu.PrefetchScalarGridSpec(
            num_scalar_prefetch=1,
            grid=(slots // step,),
            in_specs=[
                pl.BlockSpec((step, rows_dev, latitudes), lambda s, info: (first + s, 0, 0)),
                pl.BlockSpec((step, rows_dev, latitudes), lambda s, info: (s, 0, 0)),
                pl.BlockSpec((step, rows_dev, width), lambda s, info: (s, 0, 0)),
                pl.BlockSpec((step, rows_dev, width), lambda s, info: (s, 0, 0)),
            ],
            out_specs=[pl.BlockSpec(shape, lambda s, info: (0, 0, 0, 0)) for _ in range(far)],
            scratch_shapes=[pltpu.VMEM((width // LANES, latitudes * slots, LANES), F32)],
        ),
        out_shape=[jax.ShapeDtypeStruct(shape, BF16) for _ in range(far)],
        compiler_params=params("arbitrary"),
        cost_estimate=cost(16 * slots * rows_dev * latitudes * width, 8 * slots * rows_dev * width),
        name="legendre_fwd",
    )(info, leg_own, leg_other, own, recv)


def legendre_adj_body(info, lo, lx, *rest):
    bands, (own, send, scratch) = rest[:-3], rest[-3:]
    inner, lats, slots, width = bands[0].shape
    far = len(bands)
    step = own.shape[0]

    @pl.when(pl.program_id(0) == 0)
    def _():
        for shift, band in enumerate(bands):
            base = (info[1] + shift) % far * inner

            @pl.loop(0, inner)
            def _(near):
                start = pl.multiple_of((base + near) * lats * slots, lats * slots)
                for tile in range(width // LANES):
                    rows = band[near, :, :, tile * LANES : (tile + 1) * LANES].reshape(lats * slots, LANES)
                    scratch[tile, pl.ds(start, lats * slots), :] = rows.astype(F32)

    for i in range(step):
        slot = pl.program_id(0) * step + i
        rows = jnp.concatenate(
            [
                scratch[tile, pl.ds(slot, far * inner * lats, stride=slots), :]
                for tile in range(width // LANES)
            ],
            axis=1,
        ).astype(BF16)
        own[i] = dot(lo[i], rows, ((1,), (0,))).astype(BF16)
        send[i] = dot(lx[i], rows, ((1,), (0,))).astype(BF16)


def legendre_adj(leg_own, leg_other, bands, info, first_slot):
    _, rows_dev, latitudes = leg_own.shape
    slots, width = bands[0].shape[2:]
    step = STEP if slots % STEP == 0 else 1
    first = first_slot // step
    col = pl.BlockSpec((step, rows_dev, width), lambda s, info: (s, 0, 0))
    shape = jax.ShapeDtypeStruct((slots, rows_dev, width), BF16)
    return pl.pallas_call(
        legendre_adj_body,
        grid_spec=pltpu.PrefetchScalarGridSpec(
            num_scalar_prefetch=1,
            grid=(slots // step,),
            in_specs=[
                pl.BlockSpec((step, rows_dev, latitudes), lambda s, info: (first + s, 0, 0)),
                pl.BlockSpec((step, rows_dev, latitudes), lambda s, info: (s, 0, 0)),
            ]
            + [pl.BlockSpec(band.shape, lambda s, info: (0, 0, 0, 0)) for band in bands],
            out_specs=[col, col],
            scratch_shapes=[pltpu.VMEM((width // LANES, latitudes * slots, LANES), F32)],
        ),
        out_shape=[shape, shape],
        compiler_params=params("arbitrary"),
        cost_estimate=cost(16 * slots * rows_dev * latitudes * width, 8 * slots * rows_dev * width),
        name="legendre_adj",
    )(info, leg_own, leg_other, *bands)


def table_body(points, waves, cosine, sine):
    count_i = points[pl.program_id(0)]
    count = jnp.full((1, 1), count_i, jnp.int32).astype(F32)
    inverse = 1.0 / count
    wave = waves[...]
    lon_i = lax.broadcasted_iota(jnp.int32, cosine.shape[1:], 1)
    product = wave * lon_i.astype(F32)
    rest = product - jnp.floor(product * inverse) * count
    rest = jnp.where(rest < 0.0, rest + count, rest)
    rest = jnp.where(rest >= count, rest - count, rest)
    quarters = rest * (4.0 * inverse)
    whole = jnp.floor(quarters + 0.5)
    x = (quarters - whole) * (0.5 * math.pi)
    y = x * x
    s = x * (1.0 + y * (-1.0 / 6 + y * (1.0 / 120 + y * (-1.0 / 5040 + y * (1.0 / 362880)))))
    c = 1.0 + y * (-0.5 + y * (1.0 / 24 + y * (-1.0 / 720 + y * (1.0 / 40320))))
    turn = whole.astype(jnp.int32)
    odd = (turn & 1) != 0
    factor = jnp.where(wave == 0.0, 1.0, 2.0) / math.sqrt(4.0 * WAVES)
    factor = jnp.where(lon_i < count_i, factor, 0.0)
    cos_factor = jnp.where(((turn + 1) & 2) != 0, -factor, factor)
    sin_factor = jnp.where((turn & 2) != 0, factor, -factor)
    cosine[0] = (cos_factor * jnp.where(odd, s, c)).astype(BF16)
    sine[0] = (sin_factor * jnp.where(odd, c, s)).astype(BF16)


def fourier_tables(points, wave_of_slot):
    lats, count = points.shape[0], wave_of_slot.shape[0]
    shape = jax.ShapeDtypeStruct((lats, count, LONGITUDES), BF16)
    block = pl.BlockSpec((1, count, LONGITUDES), lambda t, n: (t, 0, 0))
    return pl.pallas_call(
        table_body,
        grid_spec=pltpu.PrefetchScalarGridSpec(
            num_scalar_prefetch=1,
            grid=(lats,),
            in_specs=[pl.BlockSpec((count, 1), lambda t, n: (0, 0))],
            out_specs=[block, block],
        ),
        out_shape=[shape, shape],
        compiler_params=params("arbitrary"),
        cost_estimate=cost(40 * lats * count * LONGITUDES, 4 * lats * count * LONGITUDES),
        name="fourier_tables",
    )(points, wave_of_slot.astype(F32)[:, None])


def grid_body(by_lat, cosine, sine, scale, weight, *rest):
    increment, adjoint = rest[-2:]
    groups, _, slots, width = by_lat.shape
    half = width // 2
    rows = by_lat[:, 0].reshape(groups * slots, width)
    synthesis = dot(rows[:, :half], cosine[0], ((0,), (0,)))
    synthesis = synthesis + dot(rows[:, half:], sine[0], ((0,), (0,)))
    lat_scale = scale[0]
    inc = (synthesis * lat_scale).astype(BF16)
    increment[0, 0] = inc
    weighted = (inc.astype(F32) * weight[0].astype(F32) * lat_scale).astype(BF16)
    for part, table in ((0, cosine), (1, sine)):
        total = dot(table[0], weighted, ((1,), (1,))).astype(BF16)
        adjoint[:, 0, :, part * half : (part + 1) * half] = total.reshape(groups, slots, half)


def grid_stage(by_lat, tables, lat_scale, obs_weight, member, sub, shape, into):
    groups, lats, slots, width = by_lat.shape
    half = width // 2
    count = groups * slots
    table = pl.BlockSpec((1, count, LONGITUDES), lambda t: (t, 0, 0))
    lat_rows = pl.BlockSpec((groups, 1, slots, width), lambda t: (0, t, 0, 0))
    in_specs = [
        lat_rows,
        table,
        table,
        pl.BlockSpec((1, half, 1), lambda t: (t, sub, 0)),
        pl.BlockSpec((1, half, LONGITUDES), lambda t: (t, sub, 0)),
    ]
    operands = [by_lat, *tables, lat_scale, obs_weight]
    aliases = {}
    if into is not None:
        in_specs.append(pl.BlockSpec(memory_space=pl.ANY))
        operands.append(into)
        aliases = {5: 0}
    return pl.pallas_call(
        grid_body,
        grid=(lats,),
        in_specs=in_specs,
        out_specs=[
            pl.BlockSpec((1, 1, half, LONGITUDES), lambda t: (member, t, sub, 0)),
            lat_rows,
        ],
        out_shape=[jax.ShapeDtypeStruct(shape, BF16), jax.ShapeDtypeStruct(by_lat.shape, BF16)],
        input_output_aliases=aliases,
        compiler_params=params("arbitrary"),
        cost_estimate=cost(4 * lats * count * LONGITUDES * width, 6 * lats * count * LONGITUDES),
        name="grid_stage",
    )(*operands)


def swap(values):
    return lax.ppermute(values, "lev", [(0, 1), (1, 0)])


def near_exchange(values, far, inner):
    runs = [[i * inner + j for j in range(inner)] for i in range(far)]
    return lax.all_to_all(values, "wave", split_axis=0, concat_axis=0, axis_index_groups=runs, tiled=True)


def far_shift(values, shift, far, inner):
    count = far * inner
    return lax.ppermute(values, "wave", [(i, (i + shift * inner) % count) for i in range(count)])


def chunked(control, wave_of_slot, legendre, vertical, points, lat_band, grid_scale, obs_weight):
    members, slots, _ = control.shape[:3]
    groups = legendre.shape[2] // points.shape[0]
    inner = NEAR if groups % NEAR == 0 else 1
    far = groups // inner
    lats, col_dev, _ = obs_weight.shape
    subs = col_dev // LEVELS
    half = slots // 2
    grid_shape = (members, lats, col_dev, LONGITUDES)
    place = lax.axis_index("wave").astype(jnp.int32)
    run = place // inner
    info = jnp.stack([lax.axis_index("lev").astype(jnp.int32), run])
    waves = lax.dynamic_slice_in_dim(wave_of_slot, place * slots, slots)
    sources = (run - jnp.arange(far, dtype=jnp.int32)) % far
    by_run = wave_of_slot.reshape(far, inner, slots)[sources]
    arrival_waves = jnp.swapaxes(by_run, 0, 1).reshape(-1)
    chooser = (
        lat_band[:, None] == jnp.arange(grid_scale.shape[0], dtype=jnp.int32)[None, :]
    ).astype(F32)
    lat_scale = jnp.dot(chooser, grid_scale, precision=lax.Precision.HIGHEST)[:, :, None]
    chunks = [(member, sub) for member in range(members) for sub in range(subs)]
    last = len(chunks) - 1
    whole = [(q, 0, slots) for q in range(len(chunks))]
    units_out = [(0, 0, half), (0, half, half)] + whole[1:]
    units_back = whole[:-1] + [(last, 0, half), (last, half, half)]

    leg_parts = []
    for first in (0, half):
        leg_parts.append(swap(legendre[first : first + half]))
    fields = []
    for q, first, count in units_out:
        member, sub = chunks[q]
        sent = vertical_fwd(control, vertical, info, waves, (member, sub, subs, True), first, count)
        recv = swap(sent)
        own = vertical_fwd(control, vertical, info, waves, (member, sub, subs, False), first, count)
        fields.append((own, recv))
    tables = fourier_tables(points, arrival_waves)
    leg_other = jnp.concatenate(leg_parts, axis=0)

    arrived = [[] for _ in chunks]
    for (q, first, count), (own, recv) in zip(units_out, fields):
        partner = leg_other if count == slots else leg_parts[first // half]
        pieces = list(legendre_fwd(legendre, partner, own, recv, info, far, inner, first))
        pieces = pieces[:1] + [far_shift(pieces[r], r, far, inner) for r in range(1, far)]
        arrived[q].append(near_exchange(jnp.stack(pieces, axis=1), far, inner))
    increment = gradient = None
    adjoints = []
    for q, (member, sub) in enumerate(chunks):
        by_lat = arrived[q][0] if len(arrived[q]) == 1 else jnp.concatenate(arrived[q], axis=3)
        by_lat = by_lat.reshape(groups, lats, slots, by_lat.shape[-1])
        increment, adjoint = grid_stage(
            by_lat, tables, lat_scale, obs_weight, member, sub, grid_shape, increment
        )
        adjoints.append(adjoint)
    for q, first, count in units_back:
        member, sub = chunks[q]
        partner = leg_other if count == slots else leg_parts[first // half]
        near = adjoints[q] if count == slots else adjoints[q][:, :, first : first + count]
        near = near_exchange(near.reshape(inner, far, *near.shape[1:]), far, inner)
        bands = [near[:, 0]] + [far_shift(near[:, r], -r, far, inner) for r in range(1, far)]
        own, sent = legendre_adj(legendre, partner, bands, info, first)
        recv = swap(sent)
        for block, other in ((own, False), (recv, True)):
            gradient = vertical_adj(
                block, vertical, info, waves, (member, sub, subs, other), first, control.shape, gradient
            )
    return (increment, gradient)


def fourier_table(wave_ids, lat_points):
    lon_index = jnp.arange(LONGITUDES, dtype=jnp.int32)
    remainder = wave_ids[None, :, None] * lon_index[None, None, :] % lat_points[:, None, None]
    angles = (
        2.0
        * math.pi
        * remainder.astype(jnp.float32)
        / lat_points.astype(jnp.float32)[:, None, None]
    )
    factor = jnp.where(wave_ids == 0, 1.0, 2.0).astype(jnp.float32) / math.sqrt(4.0 * WAVES)
    inside = lon_index[None, None, :] < lat_points[:, None, None]
    cosine = jnp.where(inside, factor[None, :, None] * jnp.cos(angles), 0.0)
    sine = jnp.where(inside, -factor[None, :, None] * jnp.sin(angles), 0.0)
    return jnp.stack([cosine, sine], axis=2).astype(jnp.bfloat16)


def vertical_apply(field, vertical, live_rows, band_of, forward):
    members, slots, rows_dev = (field.shape[0], field.shape[1], field.shape[2])
    shaped = field.reshape(members, slots, rows_dev, 2, VARIABLES, LEVELS)
    form = "eskpam,alm->eskpal" if forward else "eskpal,alm->eskpam"
    summed = jnp.zeros(shaped.shape, jnp.float32)
    for index_band in range(COV_BANDS):
        partial_value = jnp.einsum(
            form, shaped, vertical[index_band], preferred_element_type=jnp.float32
        )
        chosen = live_rows & (band_of == index_band)
        summed = summed + jnp.where(chosen[None, :, :, None, None, None], partial_value, 0.0)
    return summed.reshape(field.shape).astype(jnp.bfloat16)


def to_bands(values):
    return lax.all_to_all(values, "wave", split_axis=2, concat_axis=1, tiled=True)


def shards(control, wave_of_slot, legendre, vertical, points, lat_band, grid_scale, obs_weight):
    members, slots, rows_dev = (control.shape[0], control.shape[1], control.shape[2])
    slot_start = lax.axis_index("wave") * slots
    row_start = lax.axis_index("lev") * rows_dev
    own_waves = lax.dynamic_slice_in_dim(wave_of_slot, slot_start, slots)
    row_index = row_start + jnp.arange(rows_dev, dtype=jnp.int32)
    totals_n = own_waves[:, None] + row_index[None, :]
    live_rows = totals_n <= WAVES - 1
    band_of = jnp.minimum(totals_n * COV_BANDS // WAVES, COV_BANDS - 1)
    spectral = vertical_apply(control, vertical, live_rows, band_of, True)
    columns = lax.all_to_all(spectral, "lev", split_axis=4, concat_axis=2, tiled=True)
    col_dev = columns.shape[4]
    width = 2 * col_dev
    all_rows = columns.shape[2]
    columns = columns.reshape(members, slots, all_rows, width)
    coeffs = jnp.einsum(
        "skt,eskq->estq",
        lax.all_gather(legendre, "lev", axis=1, tiled=True),
        columns,
        preferred_element_type=jnp.float32,
    )
    coeffs = coeffs.astype(jnp.bfloat16)
    by_lat = to_bands(coeffs)
    wave_count = by_lat.shape[1]
    lat_dev = by_lat.shape[2]
    by_lat = by_lat.reshape(members, wave_count, lat_dev, 2, col_dev)
    fourier = fourier_table(wave_of_slot, points)
    synthesis = jnp.einsum("tspj,estpc->etcj", fourier, by_lat, preferred_element_type=jnp.float32)
    chooser = (
        lat_band[:, None] == jnp.arange(grid_scale.shape[0], dtype=jnp.int32)[None, :]
    ).astype(jnp.float32)
    lat_scale = jnp.dot(chooser, grid_scale, precision=lax.Precision.HIGHEST)
    increment = (synthesis * lat_scale[None, :, :, None]).astype(jnp.bfloat16)
    weighted = (
        increment.astype(jnp.float32) * obs_weight.astype(jnp.float32) * lat_scale[None, :, :, None]
    ).astype(jnp.bfloat16)
    adjoint_fourier = jnp.einsum(
        "tspj,etcj->etspc", fourier, weighted, preferred_element_type=jnp.float32
    )
    adjoint_fourier = adjoint_fourier.astype(jnp.bfloat16).reshape(
        members, lat_dev, wave_count, width
    )
    band_rows = to_bands(adjoint_fourier)
    adjoint_coeffs = jnp.einsum(
        "skt,etsq->eskq",
        lax.all_gather(legendre, "lev", axis=1, tiled=True),
        band_rows,
        preferred_element_type=jnp.float32,
    )
    adjoint_coeffs = adjoint_coeffs.astype(jnp.bfloat16).reshape(
        members, slots, all_rows, 2, col_dev
    )
    rows_back = lax.all_to_all(adjoint_coeffs, "lev", split_axis=2, concat_axis=4, tiled=True)
    gradient = vertical_apply(rows_back, vertical, live_rows, band_of, False)
    return (increment, gradient)


def solution(mesh):
    in_specs = (
        P(None, "wave", "lev", None, None),
        P(),
        P("wave", "lev", None),
        P(),
        P("wave"),
        P("wave"),
        P(None, "lev"),
        P("wave", "lev", None),
    )
    out_specs = (P(None, "wave", "lev", None), P(None, "wave", "lev", None, None))

    def body(control, *rest):
        levs = mesh.shape["lev"]
        slots, rows_dev = control.shape[1:3]
        whole_blocks = slots % 16 == 0 and rows_dev % 16 == 0 and rest[3].shape[0] % 16 == 0
        if levs == 2 and control.shape[4] % (levs * LEVELS) == 0 and whole_blocks:
            return chunked(control, *rest)
        return shards(control, *rest)

    return jax.shard_map(body, mesh=mesh, in_specs=in_specs, out_specs=out_specs, check_vma=False)
```

```python
import functools
import math

import jax
import jax.numpy as jnp
from jax import lax
from jax.experimental import pallas as pl
from jax.experimental.pallas import tpu as pltpu
from jax.sharding import PartitionSpec as P


WAVES = 256
LONGITUDES = 512
LEVELS = 128
VARIABLES = 4
COV_BANDS = 4
LANES = 128
STEP = 4
NEAR = 4


BF16 = jnp.bfloat16
F32 = jnp.float32


def params(*semantics):
    return pltpu.CompilerParams(dimension_semantics=semantics, vmem_limit_bytes=56 << 20)


def cost(flops, nbytes):
    return pl.CostEstimate(flops=int(flops), bytes_accessed=int(nbytes), transcendentals=0)


def dot(a, b, contract):
    return lax.dot_general(a, b, (contract, ((), ())), preferred_element_type=F32)


def band_masks(count, first_total):
    row_total = first_total + (lax.broadcasted_iota(jnp.int32, (count, LEVELS), 0) >> 1)
    width = WAVES // COV_BANDS
    masks = []
    for band in range(COV_BANDS):
        inside = (row_total >= band * width) & (row_total < (band + 1) * width)
        masks.append(jnp.where(inside, 1.0, 0.0).astype(BF16))
    return masks


def band_rows_of(rows, first_total):
    return jnp.concatenate([rows * mask for mask in band_masks(rows.shape[0], first_total)], axis=1)


def vertical_fwd_body(first_slot, info, waves, x, v, out, dense, scratch):
    step, rows_dev = out.shape[:2]
    matrix = jnp.concatenate([v[band, 0] for band in range(COV_BANDS)], axis=1)

    @pl.loop(0, step)
    def _(i):
        slot = first_slot + pl.program_id(0) * step + i
        first_total = waves[slot] + info[0] * rows_dev
        dense[...] = x[0, i].reshape(2 * rows_dev, LEVELS)
        scratch[...] = dot(band_rows_of(dense[...], first_total), matrix, ((1,), (1,)))
        for part in range(2):
            out[i, :, part * LEVELS : (part + 1) * LEVELS] = scratch[
                pl.ds(part, rows_dev, stride=2), :
            ].astype(BF16)


def column_of(info, sub, subs, other):
    lev = (1 - info[0]) if other else info[0]
    return lev * subs + sub


def vertical_fwd(control, vertical, info, waves, where, first_slot, slots):
    member, sub, subs, other = where
    rows_dev = control.shape[2]
    step = STEP if slots % STEP == 0 else 1
    first = first_slot // step
    column = lambda info: column_of(info, sub, subs, other)
    return pl.pallas_call(
        functools.partial(vertical_fwd_body, first_slot),
        grid_spec=pltpu.PrefetchScalarGridSpec(
            num_scalar_prefetch=2,
            grid=(slots // step,),
            in_specs=[
                pl.BlockSpec(
                    (1, step, rows_dev, 2, LEVELS), lambda s, info, w: (member, first + s, 0, 0, column(info))
                ),
                pl.BlockSpec((COV_BANDS, 1, LEVELS, LEVELS), lambda s, info, w: (0, column(info), 0, 0)),
            ],
            out_specs=pl.BlockSpec((step, rows_dev, 2 * LEVELS), lambda s, info, w: (s, 0, 0)),
            scratch_shapes=[
                pltpu.VMEM((2 * rows_dev, LEVELS), BF16),
                pltpu.VMEM((2 * rows_dev, LEVELS), F32),
            ],
        ),
        out_shape=jax.ShapeDtypeStruct((slots, rows_dev, 2 * LEVELS), BF16),
        compiler_params=params("arbitrary"),
        cost_estimate=cost(64 * slots * rows_dev * COV_BANDS * LEVELS * LEVELS, 8 * slots * rows_dev * 256),
        name="vertical_fwd",
    )(info, waves, control, vertical)


def vertical_adj_body(first_slot, info, waves, block, v, *rest):
    out, scratch = rest[-2:]
    step, rows_dev = block.shape[:2]
    matrix = v[:, 0].reshape(COV_BANDS * LEVELS, LEVELS)

    @pl.loop(0, step)
    def _(i):
        slot = first_slot + pl.program_id(0) * step + i
        first_total = waves[slot] + info[0] * rows_dev
        for part in range(2):
            scratch[pl.ds(part, rows_dev, stride=2), :] = block[
                i, :, part * LEVELS : (part + 1) * LEVELS
            ].astype(F32)
        rows = scratch[...].astype(BF16)
        total = dot(band_rows_of(rows, first_total), matrix, ((1,), (0,)))
        out[0, i] = total.astype(BF16).reshape(rows_dev, 2, LEVELS)


def vertical_adj(block, vertical, info, waves, where, first_slot, shape, into):
    member, sub, subs, other = where
    slots, rows_dev, width = block.shape
    step = STEP if slots % STEP == 0 else 1
    first = first_slot // step
    column = lambda info: column_of(info, sub, subs, other)
    in_specs = [
        pl.BlockSpec((step, rows_dev, width), lambda s, info, w: (s, 0, 0)),
        pl.BlockSpec((COV_BANDS, 1, LEVELS, LEVELS), lambda s, info, w: (0, column(info), 0, 0)),
    ]
    operands = [info, waves, block, vertical]
    aliases = {}
    if into is not None:
        in_specs.append(pl.BlockSpec(memory_space=pl.ANY))
        operands.append(into)
        aliases = {4: 0}
    return pl.pallas_call(
        functools.partial(vertical_adj_body, first_slot),
        grid_spec=pltpu.PrefetchScalarGridSpec(
            num_scalar_prefetch=2,
            grid=(slots // step,),
            in_specs=in_specs,
            out_specs=pl.BlockSpec(
                (1, step, rows_dev, 2, LEVELS), lambda s, info, w: (member, first + s, 0, 0, column(info))
            ),
            scratch_shapes=[pltpu.VMEM((2 * rows_dev, LEVELS), F32)],
        ),
        out_shape=jax.ShapeDtypeStruct(shape, BF16),
        input_output_aliases=aliases,
        compiler_params=params("arbitrary"),
        cost_estimate=cost(64 * slots * rows_dev * COV_BANDS * LEVELS * LEVELS, 8 * slots * rows_dev * 256),
        name="vertical_adj",
    )(*operands)


def legendre_fwd_body(info, lo, lx, own, recv, *rest):
    outs, scratch = rest[:-1], rest[-1]
    inner, lats, slots, width = outs[0].shape
    far = len(outs)
    step = own.shape[0]
    for i in range(step):
        slot = pl.program_id(0) * step + i
        total = dot(lo[i], own[i], ((0,), (0,))) + dot(lx[i], recv[i], ((0,), (0,)))
        for tile in range(width // LANES):
            scratch[tile, pl.ds(slot, far * inner * lats, stride=slots), :] = total[
                :, tile * LANES : (tile + 1) * LANES
            ]

    @pl.when(pl.program_id(0) == slots // step - 1)
    def _():
        for shift, out in enumerate(outs):
            base = (info[1] + shift) % far * inner

            @pl.loop(0, inner)
            def _(near):
                start = pl.multiple_of((base + near) * lats * slots, lats * slots)
                for tile in range(width // LANES):
                    rows = scratch[tile, pl.ds(start, lats * slots), :]
                    out[near, :, :, tile * LANES : (tile + 1) * LANES] = rows.astype(BF16).reshape(
                        lats, slots, LANES
                    )


def legendre_fwd(leg_own, leg_other, own, recv, info, far, inner, first_slot):
    slots, rows_dev, width = own.shape
    latitudes = leg_own.shape[2]
    step = STEP if slots % STEP == 0 else 1
    first = first_slot // step
    lats = latitudes // (far * inner)
    shape = (inner, lats, slots, width)
    return pl.pallas_call(
        legendre_fwd_body,
        grid_spec=pltpu.PrefetchScalarGridSpec(
            num_scalar_prefetch=1,
            grid=(slots // step,),
            in_specs=[
                pl.BlockSpec((step, rows_dev, latitudes), lambda s, info: (first + s, 0, 0)),
                pl.BlockSpec((step, rows_dev, latitudes), lambda s, info: (s, 0, 0)),
                pl.BlockSpec((step, rows_dev, width), lambda s, info: (s, 0, 0)),
                pl.BlockSpec((step, rows_dev, width), lambda s, info: (s, 0, 0)),
            ],
            out_specs=[pl.BlockSpec(shape, lambda s, info: (0, 0, 0, 0)) for _ in range(far)],
            scratch_shapes=[pltpu.VMEM((width // LANES, latitudes * slots, LANES), F32)],
        ),
        out_shape=[jax.ShapeDtypeStruct(shape, BF16) for _ in range(far)],
        compiler_params=params("arbitrary"),
        cost_estimate=cost(16 * slots * rows_dev * latitudes * width, 8 * slots * rows_dev * width),
        name="legendre_fwd",
    )(info, leg_own, leg_other, own, recv)


def legendre_adj_body(info, lo, lx, *rest):
    bands, (own, send, scratch) = rest[:-3], rest[-3:]
    inner, lats, slots, width = bands[0].shape
    far = len(bands)
    step = own.shape[0]

    @pl.when(pl.program_id(0) == 0)
    def _():
        for shift, band in enumerate(bands):
            base = (info[1] + shift) % far * inner

            @pl.loop(0, inner)
            def _(near):
                start = pl.multiple_of((base + near) * lats * slots, lats * slots)
                for tile in range(width // LANES):
                    rows = band[near, :, :, tile * LANES : (tile + 1) * LANES].reshape(lats * slots, LANES)
                    scratch[tile, pl.ds(start, lats * slots), :] = rows.astype(F32)

    for i in range(step):
        slot = pl.program_id(0) * step + i
        rows = jnp.concatenate(
            [
                scratch[tile, pl.ds(slot, far * inner * lats, stride=slots), :]
                for tile in range(width // LANES)
            ],
            axis=1,
        ).astype(BF16)
        own[i] = dot(lo[i], rows, ((1,), (0,))).astype(BF16)
        send[i] = dot(lx[i], rows, ((1,), (0,))).astype(BF16)


def legendre_adj(leg_own, leg_other, bands, info, first_slot):
    _, rows_dev, latitudes = leg_own.shape
    slots, width = bands[0].shape[2:]
    step = STEP if slots % STEP == 0 else 1
    first = first_slot // step
    col = pl.BlockSpec((step, rows_dev, width), lambda s, info: (s, 0, 0))
    shape = jax.ShapeDtypeStruct((slots, rows_dev, width), BF16)
    return pl.pallas_call(
        legendre_adj_body,
        grid_spec=pltpu.PrefetchScalarGridSpec(
            num_scalar_prefetch=1,
            grid=(slots // step,),
            in_specs=[
                pl.BlockSpec((step, rows_dev, latitudes), lambda s, info: (first + s, 0, 0)),
                pl.BlockSpec((step, rows_dev, latitudes), lambda s, info: (s, 0, 0)),
            ]
            + [pl.BlockSpec(band.shape, lambda s, info: (0, 0, 0, 0)) for band in bands],
            out_specs=[col, col],
            scratch_shapes=[pltpu.VMEM((width // LANES, latitudes * slots, LANES), F32)],
        ),
        out_shape=[shape, shape],
        compiler_params=params("arbitrary"),
        cost_estimate=cost(16 * slots * rows_dev * latitudes * width, 8 * slots * rows_dev * width),
        name="legendre_adj",
    )(info, leg_own, leg_other, *bands)


def table_body(points, waves, cosine, sine):
    count_i = points[pl.program_id(0)]
    count = jnp.full((1, 1), count_i, jnp.int32).astype(F32)
    inverse = 1.0 / count
    wave = waves[...]
    lon_i = lax.broadcasted_iota(jnp.int32, cosine.shape[1:], 1)
    product = wave * lon_i.astype(F32)
    rest = product - jnp.floor(product * inverse) * count
    rest = jnp.where(rest < 0.0, rest + count, rest)
    rest = jnp.where(rest >= count, rest - count, rest)
    quarters = rest * (4.0 * inverse)
    whole = jnp.floor(quarters + 0.5)
    x = (quarters - whole) * (0.5 * math.pi)
    y = x * x
    s = x * (1.0 + y * (-1.0 / 6 + y * (1.0 / 120 + y * (-1.0 / 5040 + y * (1.0 / 362880)))))
    c = 1.0 + y * (-0.5 + y * (1.0 / 24 + y * (-1.0 / 720 + y * (1.0 / 40320))))
    turn = whole.astype(jnp.int32)
    odd = (turn & 1) != 0
    factor = jnp.where(wave == 0.0, 1.0, 2.0) / math.sqrt(4.0 * WAVES)
    factor = jnp.where(lon_i < count_i, factor, 0.0)
    cos_factor = jnp.where(((turn + 1) & 2) != 0, -factor, factor)
    sin_factor = jnp.where((turn & 2) != 0, factor, -factor)
    cosine[0] = (cos_factor * jnp.where(odd, s, c)).astype(BF16)
    sine[0] = (sin_factor * jnp.where(odd, c, s)).astype(BF16)


def fourier_tables(points, wave_of_slot):
    lats, count = points.shape[0], wave_of_slot.shape[0]
    shape = jax.ShapeDtypeStruct((lats, count, LONGITUDES), BF16)
    block = pl.BlockSpec((1, count, LONGITUDES), lambda t, n: (t, 0, 0))
    return pl.pallas_call(
        table_body,
        grid_spec=pltpu.PrefetchScalarGridSpec(
            num_scalar_prefetch=1,
            grid=(lats,),
            in_specs=[pl.BlockSpec((count, 1), lambda t, n: (0, 0))],
            out_specs=[block, block],
        ),
        out_shape=[shape, shape],
        compiler_params=params("arbitrary"),
        cost_estimate=cost(40 * lats * count * LONGITUDES, 4 * lats * count * LONGITUDES),
        name="fourier_tables",
    )(points, wave_of_slot.astype(F32)[:, None])


def grid_body(by_lat, cosine, sine, scale, weight, *rest):
    increment, adjoint = rest[-2:]
    groups, _, slots, width = by_lat.shape
    half = width // 2
    rows = by_lat[:, 0].reshape(groups * slots, width)
    synthesis = dot(rows[:, :half], cosine[0], ((0,), (0,)))
    synthesis = synthesis + dot(rows[:, half:], sine[0], ((0,), (0,)))
    lat_scale = scale[0]
    inc = (synthesis * lat_scale).astype(BF16)
    increment[0, 0] = inc
    weighted = (inc.astype(F32) * weight[0].astype(F32) * lat_scale).astype(BF16)
    for part, table in ((0, cosine), (1, sine)):
        total = dot(table[0], weighted, ((1,), (1,))).astype(BF16)
        adjoint[:, 0, :, part * half : (part + 1) * half] = total.reshape(groups, slots, half)


def grid_stage(by_lat, tables, lat_scale, obs_weight, member, sub, shape, into):
    groups, lats, slots, width = by_lat.shape
    half = width // 2
    count = groups * slots
    table = pl.BlockSpec((1, count, LONGITUDES), lambda t: (t, 0, 0))
    lat_rows = pl.BlockSpec((groups, 1, slots, width), lambda t: (0, t, 0, 0))
    in_specs = [
        lat_rows,
        table,
        table,
        pl.BlockSpec((1, half, 1), lambda t: (t, sub, 0)),
        pl.BlockSpec((1, half, LONGITUDES), lambda t: (t, sub, 0)),
    ]
    operands = [by_lat, *tables, lat_scale, obs_weight]
    aliases = {}
    if into is not None:
        in_specs.append(pl.BlockSpec(memory_space=pl.ANY))
        operands.append(into)
        aliases = {5: 0}
    return pl.pallas_call(
        grid_body,
        grid=(lats,),
        in_specs=in_specs,
        out_specs=[
            pl.BlockSpec((1, 1, half, LONGITUDES), lambda t: (member, t, sub, 0)),
            lat_rows,
        ],
        out_shape=[jax.ShapeDtypeStruct(shape, BF16), jax.ShapeDtypeStruct(by_lat.shape, BF16)],
        input_output_aliases=aliases,
        compiler_params=params("arbitrary"),
        cost_estimate=cost(4 * lats * count * LONGITUDES * width, 6 * lats * count * LONGITUDES),
        name="grid_stage",
    )(*operands)


def swap(values):
    return lax.ppermute(values, "lev", [(0, 1), (1, 0)])


def near_exchange(values, far, inner):
    runs = [[i * inner + j for j in range(inner)] for i in range(far)]
    return lax.all_to_all(values, "wave", split_axis=0, concat_axis=0, axis_index_groups=runs, tiled=True)


def far_shift(values, shift, far, inner):
    count = far * inner
    return lax.ppermute(values, "wave", [(i, (i + shift * inner) % count) for i in range(count)])


def chunked(control, wave_of_slot, legendre, vertical, points, lat_band, grid_scale, obs_weight):
    members, slots, _ = control.shape[:3]
    groups = legendre.shape[2] // points.shape[0]
    inner = NEAR if groups % NEAR == 0 else 1
    far = groups // inner
    lats, col_dev, _ = obs_weight.shape
    subs = col_dev // LEVELS
    half = slots // 2
    grid_shape = (members, lats, col_dev, LONGITUDES)
    place = lax.axis_index("wave").astype(jnp.int32)
    run = place // inner
    info = jnp.stack([lax.axis_index("lev").astype(jnp.int32), run])
    waves = lax.dynamic_slice_in_dim(wave_of_slot, place * slots, slots)
    sources = (run - jnp.arange(far, dtype=jnp.int32)) % far
    by_run = wave_of_slot.reshape(far, inner, slots)[sources]
    arrival_waves = jnp.swapaxes(by_run, 0, 1).reshape(-1)
    chooser = (
        lat_band[:, None] == jnp.arange(grid_scale.shape[0], dtype=jnp.int32)[None, :]
    ).astype(F32)
    lat_scale = jnp.dot(chooser, grid_scale, precision=lax.Precision.HIGHEST)[:, :, None]
    chunks = [(member, sub) for member in range(members) for sub in range(subs)]
    last = len(chunks) - 1
    whole = [(q, 0, slots) for q in range(len(chunks))]
    units_out = [(0, 0, half), (0, half, half)] + whole[1:]
    units_back = whole[:-1] + [(last, 0, half), (last, half, half)]

    leg_parts = []
    for first in (0, half):
        leg_parts.append(swap(legendre[first : first + half]))
    fields = []
    for q, first, count in units_out:
        member, sub = chunks[q]
        sent = vertical_fwd(control, vertical, info, waves, (member, sub, subs, True), first, count)
        recv = swap(sent)
        own = vertical_fwd(control, vertical, info, waves, (member, sub, subs, False), first, count)
        fields.append((own, recv))
    tables = fourier_tables(points, arrival_waves)
    leg_other = jnp.concatenate(leg_parts, axis=0)

    arrived = [[] for _ in chunks]
    for (q, first, count), (own, recv) in zip(units_out, fields):
        partner = leg_other if count == slots else leg_parts[first // half]
        pieces = list(legendre_fwd(legendre, partner, own, recv, info, far, inner, first))
        pieces = pieces[:1] + [far_shift(pieces[r], r, far, inner) for r in range(1, far)]
        arrived[q].append(near_exchange(jnp.stack(pieces, axis=1), far, inner))
    increment = gradient = None
    adjoints = []
    for q, (member, sub) in enumerate(chunks):
        by_lat = arrived[q][0] if len(arrived[q]) == 1 else jnp.concatenate(arrived[q], axis=3)
        by_lat = by_lat.reshape(groups, lats, slots, by_lat.shape[-1])
        increment, adjoint = grid_stage(
            by_lat, tables, lat_scale, obs_weight, member, sub, grid_shape, increment
        )
        adjoints.append(adjoint)
    for q, first, count in units_back:
        member, sub = chunks[q]
        partner = leg_other if count == slots else leg_parts[first // half]
        near = adjoints[q] if count == slots else adjoints[q][:, :, first : first + count]
        near = near_exchange(near.reshape(inner, far, *near.shape[1:]), far, inner)
        bands = [near[:, 0]] + [far_shift(near[:, r], -r, far, inner) for r in range(1, far)]
        own, sent = legendre_adj(legendre, partner, bands, info, first)
        recv = swap(sent)
        for block, other in ((own, False), (recv, True)):
            gradient = vertical_adj(
                block, vertical, info, waves, (member, sub, subs, other), first, control.shape, gradient
            )
    return (increment, gradient)


def fourier_table(wave_ids, lat_points):
    lon_index = jnp.arange(LONGITUDES, dtype=jnp.int32)
    remainder = wave_ids[None, :, None] * lon_index[None, None, :] % lat_points[:, None, None]
    angles = (
        2.0
        * math.pi
        * remainder.astype(jnp.float32)
        / lat_points.astype(jnp.float32)[:, None, None]
    )
    factor = jnp.where(wave_ids == 0, 1.0, 2.0).astype(jnp.float32) / math.sqrt(4.0 * WAVES)
    inside = lon_index[None, None, :] < lat_points[:, None, None]
    cosine = jnp.where(inside, factor[None, :, None] * jnp.cos(angles), 0.0)
    sine = jnp.where(inside, -factor[None, :, None] * jnp.sin(angles), 0.0)
    return jnp.stack([cosine, sine], axis=2).astype(jnp.bfloat16)


def vertical_apply(field, vertical, live_rows, band_of, forward):
    members, slots, rows_dev = (field.shape[0], field.shape[1], field.shape[2])
    shaped = field.reshape(members, slots, rows_dev, 2, VARIABLES, LEVELS)
    form = "eskpam,alm->eskpal" if forward else "eskpal,alm->eskpam"
    summed = jnp.zeros(shaped.shape, jnp.float32)
    for index_band in range(COV_BANDS):
        partial_value = jnp.einsum(
            form, shaped, vertical[index_band], preferred_element_type=jnp.float32
        )
        chosen = live_rows & (band_of == index_band)
        summed = summed + jnp.where(chosen[None, :, :, None, None, None], partial_value, 0.0)
    return summed.reshape(field.shape).astype(jnp.bfloat16)


def to_bands(values):
    return lax.all_to_all(values, "wave", split_axis=2, concat_axis=1, tiled=True)


def shards(control, wave_of_slot, legendre, vertical, points, lat_band, grid_scale, obs_weight):
    members, slots, rows_dev = (control.shape[0], control.shape[1], control.shape[2])
    slot_start = lax.axis_index("wave") * slots
    row_start = lax.axis_index("lev") * rows_dev
    own_waves = lax.dynamic_slice_in_dim(wave_of_slot, slot_start, slots)
    row_index = row_start + jnp.arange(rows_dev, dtype=jnp.int32)
    totals_n = own_waves[:, None] + row_index[None, :]
    live_rows = totals_n <= WAVES - 1
    band_of = jnp.minimum(totals_n * COV_BANDS // WAVES, COV_BANDS - 1)
    spectral = vertical_apply(control, vertical, live_rows, band_of, True)
    columns = lax.all_to_all(spectral, "lev", split_axis=4, concat_axis=2, tiled=True)
    col_dev = columns.shape[4]
    width = 2 * col_dev
    all_rows = columns.shape[2]
    columns = columns.reshape(members, slots, all_rows, width)
    coeffs = jnp.einsum(
        "skt,eskq->estq",
        lax.all_gather(legendre, "lev", axis=1, tiled=True),
        columns,
        preferred_element_type=jnp.float32,
    )
    coeffs = coeffs.astype(jnp.bfloat16)
    by_lat = to_bands(coeffs)
    wave_count = by_lat.shape[1]
    lat_dev = by_lat.shape[2]
    by_lat = by_lat.reshape(members, wave_count, lat_dev, 2, col_dev)
    fourier = fourier_table(wave_of_slot, points)
    synthesis = jnp.einsum("tspj,estpc->etcj", fourier, by_lat, preferred_element_type=jnp.float32)
    chooser = (
        lat_band[:, None] == jnp.arange(grid_scale.shape[0], dtype=jnp.int32)[None, :]
    ).astype(jnp.float32)
    lat_scale = jnp.dot(chooser, grid_scale, precision=lax.Precision.HIGHEST)
    increment = (synthesis * lat_scale[None, :, :, None]).astype(jnp.bfloat16)
    weighted = (
        increment.astype(jnp.float32) * obs_weight.astype(jnp.float32) * lat_scale[None, :, :, None]
    ).astype(jnp.bfloat16)
    adjoint_fourier = jnp.einsum(
        "tspj,etcj->etspc", fourier, weighted, preferred_element_type=jnp.float32
    )
    adjoint_fourier = adjoint_fourier.astype(jnp.bfloat16).reshape(
        members, lat_dev, wave_count, width
    )
    band_rows = to_bands(adjoint_fourier)
    adjoint_coeffs = jnp.einsum(
        "skt,etsq->eskq",
        lax.all_gather(legendre, "lev", axis=1, tiled=True),
        band_rows,
        preferred_element_type=jnp.float32,
    )
    adjoint_coeffs = adjoint_coeffs.astype(jnp.bfloat16).reshape(
        members, slots, all_rows, 2, col_dev
    )
    rows_back = lax.all_to_all(adjoint_coeffs, "lev", split_axis=2, concat_axis=4, tiled=True)
    gradient = vertical_apply(rows_back, vertical, live_rows, band_of, False)
    return (increment, gradient)


def solution(mesh):
    in_specs = (
        P(None, "wave", "lev", None, None),
        P(),
        P("wave", "lev", None),
        P(),
        P("wave"),
        P("wave"),
        P(None, "lev"),
        P("wave", "lev", None),
    )
    out_specs = (P(None, "wave", "lev", None), P(None, "wave", "lev", None, None))

    def body(control, *rest):
        levs = mesh.shape["lev"]
        slots, rows_dev = control.shape[1:3]
        whole_blocks = slots % 16 == 0 and rows_dev % 16 == 0 and rest[3].shape[0] % 16 == 0
        if levs == 2 and control.shape[4] % (levs * LEVELS) == 0 and whole_blocks:
            return chunked(control, *rest)
        return shards(control, *rest)

    return jax.shard_map(body, mesh=mesh, in_specs=in_specs, out_specs=out_specs, check_vma=False)
```

```python
import functools
import math

import jax
import jax.numpy as jnp
from jax import lax
from jax.experimental import pallas as pl
from jax.experimental.pallas import tpu as pltpu
from jax.sharding import PartitionSpec as P


WAVES = 256
LONGITUDES = 512
LEVELS = 128
VARIABLES = 4
COV_BANDS = 4
LANES = 128
STEP = 4
NEAR = 4


BF16 = jnp.bfloat16
F32 = jnp.float32


def params(*semantics):
    return pltpu.CompilerParams(dimension_semantics=semantics, vmem_limit_bytes=56 << 20)


def cost(flops, nbytes):
    return pl.CostEstimate(flops=int(flops), bytes_accessed=int(nbytes), transcendentals=0)


def dot(a, b, contract):
    return lax.dot_general(a, b, (contract, ((), ())), preferred_element_type=F32)


def band_masks(count, first_total):
    row_total = first_total + (lax.broadcasted_iota(jnp.int32, (count, LEVELS), 0) >> 1)
    width = WAVES // COV_BANDS
    masks = []
    for band in range(COV_BANDS):
        inside = (row_total >= band * width) & (row_total < (band + 1) * width)
        masks.append(jnp.where(inside, 1.0, 0.0).astype(BF16))
    return masks


def band_rows_of(rows, first_total):
    return jnp.concatenate([rows * mask for mask in band_masks(rows.shape[0], first_total)], axis=1)


def vertical_fwd_body(first_slot, info, waves, x, v, out, dense, scratch):
    step, rows_dev = out.shape[:2]
    matrix = jnp.concatenate([v[band, 0] for band in range(COV_BANDS)], axis=1)

    @pl.loop(0, step)
    def _(i):
        slot = first_slot + pl.program_id(0) * step + i
        first_total = waves[slot] + info[0] * rows_dev
        dense[...] = x[0, i].reshape(2 * rows_dev, LEVELS)
        scratch[...] = dot(band_rows_of(dense[...], first_total), matrix, ((1,), (1,)))
        for part in range(2):
            out[i, :, part * LEVELS : (part + 1) * LEVELS] = scratch[
                pl.ds(part, rows_dev, stride=2), :
            ].astype(BF16)


def column_of(info, sub, subs, other):
    lev = (1 - info[0]) if other else info[0]
    return lev * subs + sub


def vertical_fwd(control, vertical, info, waves, where, first_slot, slots):
    member, sub, subs, other = where
    rows_dev = control.shape[2]
    step = STEP if slots % STEP == 0 else 1
    first = first_slot // step
    column = lambda info: column_of(info, sub, subs, other)
    return pl.pallas_call(
        functools.partial(vertical_fwd_body, first_slot),
        grid_spec=pltpu.PrefetchScalarGridSpec(
            num_scalar_prefetch=2,
            grid=(slots // step,),
            in_specs=[
                pl.BlockSpec(
                    (1, step, rows_dev, 2, LEVELS), lambda s, info, w: (member, first + s, 0, 0, column(info))
                ),
                pl.BlockSpec((COV_BANDS, 1, LEVELS, LEVELS), lambda s, info, w: (0, column(info), 0, 0)),
            ],
            out_specs=pl.BlockSpec((step, rows_dev, 2 * LEVELS), lambda s, info, w: (s, 0, 0)),
            scratch_shapes=[
                pltpu.VMEM((2 * rows_dev, LEVELS), BF16),
                pltpu.VMEM((2 * rows_dev, LEVELS), F32),
            ],
        ),
        out_shape=jax.ShapeDtypeStruct((slots, rows_dev, 2 * LEVELS), BF16),
        compiler_params=params("arbitrary"),
        cost_estimate=cost(64 * slots * rows_dev * COV_BANDS * LEVELS * LEVELS, 8 * slots * rows_dev * 256),
        name="vertical_fwd",
    )(info, waves, control, vertical)


def vertical_adj_body(first_slot, info, waves, block, v, *rest):
    out, scratch = rest[-2:]
    step, rows_dev = block.shape[:2]
    matrix = v[:, 0].reshape(COV_BANDS * LEVELS, LEVELS)

    @pl.loop(0, step)
    def _(i):
        slot = first_slot + pl.program_id(0) * step + i
        first_total = waves[slot] + info[0] * rows_dev
        for part in range(2):
            scratch[pl.ds(part, rows_dev, stride=2), :] = block[
                i, :, part * LEVELS : (part + 1) * LEVELS
            ].astype(F32)
        rows = scratch[...].astype(BF16)
        total = dot(band_rows_of(rows, first_total), matrix, ((1,), (0,)))
        out[0, i] = total.astype(BF16).reshape(rows_dev, 2, LEVELS)


def vertical_adj(block, vertical, info, waves, where, first_slot, shape, into):
    member, sub, subs, other = where
    slots, rows_dev, width = block.shape
    step = STEP if slots % STEP == 0 else 1
    first = first_slot // step
    column = lambda info: column_of(info, sub, subs, other)
    in_specs = [
        pl.BlockSpec((step, rows_dev, width), lambda s, info, w: (s, 0, 0)),
        pl.BlockSpec((COV_BANDS, 1, LEVELS, LEVELS), lambda s, info, w: (0, column(info), 0, 0)),
    ]
    operands = [info, waves, block, vertical]
    aliases = {}
    if into is not None:
        in_specs.append(pl.BlockSpec(memory_space=pl.ANY))
        operands.append(into)
        aliases = {4: 0}
    return pl.pallas_call(
        functools.partial(vertical_adj_body, first_slot),
        grid_spec=pltpu.PrefetchScalarGridSpec(
            num_scalar_prefetch=2,
            grid=(slots // step,),
            in_specs=in_specs,
            out_specs=pl.BlockSpec(
                (1, step, rows_dev, 2, LEVELS), lambda s, info, w: (member, first + s, 0, 0, column(info))
            ),
            scratch_shapes=[pltpu.VMEM((2 * rows_dev, LEVELS), F32)],
        ),
        out_shape=jax.ShapeDtypeStruct(shape, BF16),
        input_output_aliases=aliases,
        compiler_params=params("arbitrary"),
        cost_estimate=cost(64 * slots * rows_dev * COV_BANDS * LEVELS * LEVELS, 8 * slots * rows_dev * 256),
        name="vertical_adj",
    )(*operands)


def legendre_fwd_body(info, lo, lx, own, recv, *rest):
    outs, scratch = rest[:-1], rest[-1]
    inner, lats, slots, width = outs[0].shape
    far = len(outs)
    step = own.shape[0]
    for i in range(step):
        slot = pl.program_id(0) * step + i
        total = dot(lo[i], own[i], ((0,), (0,))) + dot(lx[i], recv[i], ((0,), (0,)))
        for tile in range(width // LANES):
            scratch[tile, pl.ds(slot, far * inner * lats, stride=slots), :] = total[
                :, tile * LANES : (tile + 1) * LANES
            ]

    @pl.when(pl.program_id(0) == slots // step - 1)
    def _():
        for shift, out in enumerate(outs):
            base = (info[1] + shift) % far * inner

            @pl.loop(0, inner)
            def _(near):
                start = pl.multiple_of((base + near) * lats * slots, lats * slots)
                for tile in range(width // LANES):
                    rows = scratch[tile, pl.ds(start, lats * slots), :]
                    out[near, :, :, tile * LANES : (tile + 1) * LANES] = rows.astype(BF16).reshape(
                        lats, slots, LANES
                    )


def legendre_fwd(leg_own, leg_other, own, recv, info, far, inner, first_slot):
    slots, rows_dev, width = own.shape
    latitudes = leg_own.shape[2]
    step = STEP if slots % STEP == 0 else 1
    first = first_slot // step
    lats = latitudes // (far * inner)
    shape = (inner, lats, slots, width)
    return pl.pallas_call(
        legendre_fwd_body,
        grid_spec=pltpu.PrefetchScalarGridSpec(
            num_scalar_prefetch=1,
            grid=(slots // step,),
            in_specs=[
                pl.BlockSpec((step, rows_dev, latitudes), lambda s, info: (first + s, 0, 0)),
                pl.BlockSpec((step, rows_dev, latitudes), lambda s, info: (s, 0, 0)),
                pl.BlockSpec((step, rows_dev, width), lambda s, info: (s, 0, 0)),
                pl.BlockSpec((step, rows_dev, width), lambda s, info: (s, 0, 0)),
            ],
            out_specs=[pl.BlockSpec(shape, lambda s, info: (0, 0, 0, 0)) for _ in range(far)],
            scratch_shapes=[pltpu.VMEM((width // LANES, latitudes * slots, LANES), F32)],
        ),
        out_shape=[jax.ShapeDtypeStruct(shape, BF16) for _ in range(far)],
        compiler_params=params("arbitrary"),
        cost_estimate=cost(16 * slots * rows_dev * latitudes * width, 8 * slots * rows_dev * width),
        name="legendre_fwd",
    )(info, leg_own, leg_other, own, recv)


def legendre_adj_body(info, lo, lx, *rest):
    bands, (own, send, scratch) = rest[:-3], rest[-3:]
    inner, lats, slots, width = bands[0].shape
    far = len(bands)
    step = own.shape[0]

    @pl.when(pl.program_id(0) == 0)
    def _():
        for shift, band in enumerate(bands):
            base = (info[1] + shift) % far * inner

            @pl.loop(0, inner)
            def _(near):
                start = pl.multiple_of((base + near) * lats * slots, lats * slots)
                for tile in range(width // LANES):
                    rows = band[near, :, :, tile * LANES : (tile + 1) * LANES].reshape(lats * slots, LANES)
                    scratch[tile, pl.ds(start, lats * slots), :] = rows.astype(F32)

    for i in range(step):
        slot = pl.program_id(0) * step + i
        rows = jnp.concatenate(
            [
                scratch[tile, pl.ds(slot, far * inner * lats, stride=slots), :]
                for tile in range(width // LANES)
            ],
            axis=1,
        ).astype(BF16)
        own[i] = dot(lo[i], rows, ((1,), (0,))).astype(BF16)
        send[i] = dot(lx[i], rows, ((1,), (0,))).astype(BF16)


def legendre_adj(leg_own, leg_other, bands, info, first_slot):
    _, rows_dev, latitudes = leg_own.shape
    slots, width = bands[0].shape[2:]
    step = STEP if slots % STEP == 0 else 1
    first = first_slot // step
    col = pl.BlockSpec((step, rows_dev, width), lambda s, info: (s, 0, 0))
    shape = jax.ShapeDtypeStruct((slots, rows_dev, width), BF16)
    return pl.pallas_call(
        legendre_adj_body,
        grid_spec=pltpu.PrefetchScalarGridSpec(
            num_scalar_prefetch=1,
            grid=(slots // step,),
            in_specs=[
                pl.BlockSpec((step, rows_dev, latitudes), lambda s, info: (first + s, 0, 0)),
                pl.BlockSpec((step, rows_dev, latitudes), lambda s, info: (s, 0, 0)),
            ]
            + [pl.BlockSpec(band.shape, lambda s, info: (0, 0, 0, 0)) for band in bands],
            out_specs=[col, col],
            scratch_shapes=[pltpu.VMEM((width // LANES, latitudes * slots, LANES), F32)],
        ),
        out_shape=[shape, shape],
        compiler_params=params("arbitrary"),
        cost_estimate=cost(16 * slots * rows_dev * latitudes * width, 8 * slots * rows_dev * width),
        name="legendre_adj",
    )(info, leg_own, leg_other, *bands)


def table_body(points, waves, cosine, sine):
    count_i = points[pl.program_id(0)]
    count = jnp.full((1, 1), count_i, jnp.int32).astype(F32)
    inverse = 1.0 / count
    wave = waves[...]
    lon_i = lax.broadcasted_iota(jnp.int32, cosine.shape[1:], 1)
    product = wave * lon_i.astype(F32)
    rest = product - jnp.floor(product * inverse) * count
    rest = jnp.where(rest < 0.0, rest + count, rest)
    rest = jnp.where(rest >= count, rest - count, rest)
    quarters = rest * (4.0 * inverse)
    whole = jnp.floor(quarters + 0.5)
    x = (quarters - whole) * (0.5 * math.pi)
    y = x * x
    s = x * (1.0 + y * (-1.0 / 6 + y * (1.0 / 120 + y * (-1.0 / 5040 + y * (1.0 / 362880)))))
    c = 1.0 + y * (-0.5 + y * (1.0 / 24 + y * (-1.0 / 720 + y * (1.0 / 40320))))
    turn = whole.astype(jnp.int32)
    odd = (turn & 1) != 0
    factor = jnp.where(wave == 0.0, 1.0, 2.0) / math.sqrt(4.0 * WAVES)
    factor = jnp.where(lon_i < count_i, factor, 0.0)
    cos_factor = jnp.where(((turn + 1) & 2) != 0, -factor, factor)
    sin_factor = jnp.where((turn & 2) != 0, factor, -factor)
    cosine[0] = (cos_factor * jnp.where(odd, s, c)).astype(BF16)
    sine[0] = (sin_factor * jnp.where(odd, c, s)).astype(BF16)


def fourier_tables(points, wave_of_slot):
    lats, count = points.shape[0], wave_of_slot.shape[0]
    shape = jax.ShapeDtypeStruct((lats, count, LONGITUDES), BF16)
    block = pl.BlockSpec((1, count, LONGITUDES), lambda t, n: (t, 0, 0))
    return pl.pallas_call(
        table_body,
        grid_spec=pltpu.PrefetchScalarGridSpec(
            num_scalar_prefetch=1,
            grid=(lats,),
            in_specs=[pl.BlockSpec((count, 1), lambda t, n: (0, 0))],
            out_specs=[block, block],
        ),
        out_shape=[shape, shape],
        compiler_params=params("arbitrary"),
        cost_estimate=cost(40 * lats * count * LONGITUDES, 4 * lats * count * LONGITUDES),
        name="fourier_tables",
    )(points, wave_of_slot.astype(F32)[:, None])


def grid_body(by_lat, cosine, sine, scale, weight, *rest):
    increment, adjoint = rest[-2:]
    groups, step, slots, width = by_lat.shape
    half = width // 2
    for i in range(step):
        rows = by_lat[:, i].reshape(groups * slots, width)
        synthesis = dot(rows[:, :half], cosine[i], ((0,), (0,)))
        synthesis = synthesis + dot(rows[:, half:], sine[i], ((0,), (0,)))
        lat_scale = scale[i]
        inc = (synthesis * lat_scale).astype(BF16)
        increment[0, i] = inc
        weighted = (inc.astype(F32) * weight[i].astype(F32) * lat_scale).astype(BF16)
        for part, table in ((0, cosine), (1, sine)):
            total = dot(table[i], weighted, ((1,), (1,))).astype(BF16)
            adjoint[:, i, :, part * half : (part + 1) * half] = total.reshape(groups, slots, half)


def grid_stage(by_lat, tables, lat_scale, obs_weight, member, sub, shape, into):
    groups, lats, slots, width = by_lat.shape
    half = width // 2
    count = groups * slots
    step = 2 if lats % 2 == 0 else 1
    table = pl.BlockSpec((step, count, LONGITUDES), lambda t: (t, 0, 0))
    lat_rows = pl.BlockSpec((groups, step, slots, width), lambda t: (0, t, 0, 0))
    in_specs = [
        lat_rows,
        table,
        table,
        pl.BlockSpec((step, half, 1), lambda t: (t, sub, 0)),
        pl.BlockSpec((step, half, LONGITUDES), lambda t: (t, sub, 0)),
    ]
    operands = [by_lat, *tables, lat_scale, obs_weight]
    aliases = {}
    if into is not None:
        in_specs.append(pl.BlockSpec(memory_space=pl.ANY))
        operands.append(into)
        aliases = {5: 0}
    return pl.pallas_call(
        grid_body,
        grid=(lats // step,),
        in_specs=in_specs,
        out_specs=[
            pl.BlockSpec((1, step, half, LONGITUDES), lambda t: (member, t, sub, 0)),
            lat_rows,
        ],
        out_shape=[jax.ShapeDtypeStruct(shape, BF16), jax.ShapeDtypeStruct(by_lat.shape, BF16)],
        input_output_aliases=aliases,
        compiler_params=params("arbitrary"),
        cost_estimate=cost(4 * lats * count * LONGITUDES * width, 6 * lats * count * LONGITUDES),
        name="grid_stage",
    )(*operands)


def swap(values):
    return lax.ppermute(values, "lev", [(0, 1), (1, 0)])


def near_exchange(values, far, inner):
    runs = [[i * inner + j for j in range(inner)] for i in range(far)]
    return lax.all_to_all(values, "wave", split_axis=0, concat_axis=0, axis_index_groups=runs, tiled=True)


def far_shift(values, shift, far, inner):
    count = far * inner
    return lax.ppermute(values, "wave", [(i, (i + shift * inner) % count) for i in range(count)])


def chunked(control, wave_of_slot, legendre, vertical, points, lat_band, grid_scale, obs_weight):
    members, slots, _ = control.shape[:3]
    groups = legendre.shape[2] // points.shape[0]
    inner = NEAR if groups % NEAR == 0 else 1
    far = groups // inner
    lats, col_dev, _ = obs_weight.shape
    subs = col_dev // LEVELS
    half = slots // 2
    grid_shape = (members, lats, col_dev, LONGITUDES)
    place = lax.axis_index("wave").astype(jnp.int32)
    run = place // inner
    info = jnp.stack([lax.axis_index("lev").astype(jnp.int32), run])
    waves = lax.dynamic_slice_in_dim(wave_of_slot, place * slots, slots)
    sources = (run - jnp.arange(far, dtype=jnp.int32)) % far
    by_run = wave_of_slot.reshape(far, inner, slots)[sources]
    arrival_waves = jnp.swapaxes(by_run, 0, 1).reshape(-1)
    chooser = (
        lat_band[:, None] == jnp.arange(grid_scale.shape[0], dtype=jnp.int32)[None, :]
    ).astype(F32)
    lat_scale = jnp.dot(chooser, grid_scale, precision=lax.Precision.HIGHEST)[:, :, None]
    chunks = [(member, sub) for member in range(members) for sub in range(subs)]
    last = len(chunks) - 1
    whole = [(q, 0, slots) for q in range(len(chunks))]
    units_out = [(0, 0, half), (0, half, half)] + whole[1:]
    units_back = whole[:-1] + [(last, 0, half), (last, half, half)]

    leg_parts = []
    for first in (0, half):
        leg_parts.append(swap(legendre[first : first + half]))
    fields = []
    for q, first, count in units_out:
        member, sub = chunks[q]
        sent = vertical_fwd(control, vertical, info, waves, (member, sub, subs, True), first, count)
        recv = swap(sent)
        own = vertical_fwd(control, vertical, info, waves, (member, sub, subs, False), first, count)
        fields.append((own, recv))
    tables = fourier_tables(points, arrival_waves)
    leg_other = jnp.concatenate(leg_parts, axis=0)

    arrived = [[] for _ in chunks]
    for (q, first, count), (own, recv) in zip(units_out, fields):
        partner = leg_other if count == slots else leg_parts[first // half]
        pieces = list(legendre_fwd(legendre, partner, own, recv, info, far, inner, first))
        pieces = pieces[:1] + [far_shift(pieces[r], r, far, inner) for r in range(1, far)]
        arrived[q].append(near_exchange(jnp.stack(pieces, axis=1), far, inner))
    increment = gradient = None
    adjoints = []
    for q, (member, sub) in enumerate(chunks):
        by_lat = arrived[q][0] if len(arrived[q]) == 1 else jnp.concatenate(arrived[q], axis=3)
        by_lat = by_lat.reshape(groups, lats, slots, by_lat.shape[-1])
        increment, adjoint = grid_stage(
            by_lat, tables, lat_scale, obs_weight, member, sub, grid_shape, increment
        )
        adjoints.append(adjoint)
    for q, first, count in units_back:
        member, sub = chunks[q]
        partner = leg_other if count == slots else leg_parts[first // half]
        near = adjoints[q] if count == slots else adjoints[q][:, :, first : first + count]
        near = near_exchange(near.reshape(inner, far, *near.shape[1:]), far, inner)
        bands = [near[:, 0]] + [far_shift(near[:, r], -r, far, inner) for r in range(1, far)]
        own, sent = legendre_adj(legendre, partner, bands, info, first)
        recv = swap(sent)
        for block, other in ((own, False), (recv, True)):
            gradient = vertical_adj(
                block, vertical, info, waves, (member, sub, subs, other), first, control.shape, gradient
            )
    return (increment, gradient)


def fourier_table(wave_ids, lat_points):
    lon_index = jnp.arange(LONGITUDES, dtype=jnp.int32)
    remainder = wave_ids[None, :, None] * lon_index[None, None, :] % lat_points[:, None, None]
    angles = (
        2.0
        * math.pi
        * remainder.astype(jnp.float32)
        / lat_points.astype(jnp.float32)[:, None, None]
    )
    factor = jnp.where(wave_ids == 0, 1.0, 2.0).astype(jnp.float32) / math.sqrt(4.0 * WAVES)
    inside = lon_index[None, None, :] < lat_points[:, None, None]
    cosine = jnp.where(inside, factor[None, :, None] * jnp.cos(angles), 0.0)
    sine = jnp.where(inside, -factor[None, :, None] * jnp.sin(angles), 0.0)
    return jnp.stack([cosine, sine], axis=2).astype(jnp.bfloat16)


def vertical_apply(field, vertical, live_rows, band_of, forward):
    members, slots, rows_dev = (field.shape[0], field.shape[1], field.shape[2])
    shaped = field.reshape(members, slots, rows_dev, 2, VARIABLES, LEVELS)
    form = "eskpam,alm->eskpal" if forward else "eskpal,alm->eskpam"
    summed = jnp.zeros(shaped.shape, jnp.float32)
    for index_band in range(COV_BANDS):
        partial_value = jnp.einsum(
            form, shaped, vertical[index_band], preferred_element_type=jnp.float32
        )
        chosen = live_rows & (band_of == index_band)
        summed = summed + jnp.where(chosen[None, :, :, None, None, None], partial_value, 0.0)
    return summed.reshape(field.shape).astype(jnp.bfloat16)


def to_bands(values):
    return lax.all_to_all(values, "wave", split_axis=2, concat_axis=1, tiled=True)


def shards(control, wave_of_slot, legendre, vertical, points, lat_band, grid_scale, obs_weight):
    members, slots, rows_dev = (control.shape[0], control.shape[1], control.shape[2])
    slot_start = lax.axis_index("wave") * slots
    row_start = lax.axis_index("lev") * rows_dev
    own_waves = lax.dynamic_slice_in_dim(wave_of_slot, slot_start, slots)
    row_index = row_start + jnp.arange(rows_dev, dtype=jnp.int32)
    totals_n = own_waves[:, None] + row_index[None, :]
    live_rows = totals_n <= WAVES - 1
    band_of = jnp.minimum(totals_n * COV_BANDS // WAVES, COV_BANDS - 1)
    spectral = vertical_apply(control, vertical, live_rows, band_of, True)
    columns = lax.all_to_all(spectral, "lev", split_axis=4, concat_axis=2, tiled=True)
    col_dev = columns.shape[4]
    width = 2 * col_dev
    all_rows = columns.shape[2]
    columns = columns.reshape(members, slots, all_rows, width)
    coeffs = jnp.einsum(
        "skt,eskq->estq",
        lax.all_gather(legendre, "lev", axis=1, tiled=True),
        columns,
        preferred_element_type=jnp.float32,
    )
    coeffs = coeffs.astype(jnp.bfloat16)
    by_lat = to_bands(coeffs)
    wave_count = by_lat.shape[1]
    lat_dev = by_lat.shape[2]
    by_lat = by_lat.reshape(members, wave_count, lat_dev, 2, col_dev)
    fourier = fourier_table(wave_of_slot, points)
    synthesis = jnp.einsum("tspj,estpc->etcj", fourier, by_lat, preferred_element_type=jnp.float32)
    chooser = (
        lat_band[:, None] == jnp.arange(grid_scale.shape[0], dtype=jnp.int32)[None, :]
    ).astype(jnp.float32)
    lat_scale = jnp.dot(chooser, grid_scale, precision=lax.Precision.HIGHEST)
    increment = (synthesis * lat_scale[None, :, :, None]).astype(jnp.bfloat16)
    weighted = (
        increment.astype(jnp.float32) * obs_weight.astype(jnp.float32) * lat_scale[None, :, :, None]
    ).astype(jnp.bfloat16)
    adjoint_fourier = jnp.einsum(
        "tspj,etcj->etspc", fourier, weighted, preferred_element_type=jnp.float32
    )
    adjoint_fourier = adjoint_fourier.astype(jnp.bfloat16).reshape(
        members, lat_dev, wave_count, width
    )
    band_rows = to_bands(adjoint_fourier)
    adjoint_coeffs = jnp.einsum(
        "skt,etsq->eskq",
        lax.all_gather(legendre, "lev", axis=1, tiled=True),
        band_rows,
        preferred_element_type=jnp.float32,
    )
    adjoint_coeffs = adjoint_coeffs.astype(jnp.bfloat16).reshape(
        members, slots, all_rows, 2, col_dev
    )
    rows_back = lax.all_to_all(adjoint_coeffs, "lev", split_axis=2, concat_axis=4, tiled=True)
    gradient = vertical_apply(rows_back, vertical, live_rows, band_of, False)
    return (increment, gradient)


def solution(mesh):
    in_specs = (
        P(None, "wave", "lev", None, None),
        P(),
        P("wave", "lev", None),
        P(),
        P("wave"),
        P("wave"),
        P(None, "lev"),
        P("wave", "lev", None),
    )
    out_specs = (P(None, "wave", "lev", None), P(None, "wave", "lev", None, None))

    def body(control, *rest):
        levs = mesh.shape["lev"]
        slots, rows_dev = control.shape[1:3]
        whole_blocks = slots % 16 == 0 and rows_dev % 16 == 0 and rest[3].shape[0] % 16 == 0
        if levs == 2 and control.shape[4] % (levs * LEVELS) == 0 and whole_blocks:
            return chunked(control, *rest)
        return shards(control, *rest)

    return jax.shard_map(body, mesh=mesh, in_specs=in_specs, out_specs=out_specs, check_vma=False)
```
